256 devices in a mesh: ep: 64 (over z, y, core), fsdp: 4 (over x).
Axes of the slice: x: 4, y: 4, z: 8, core: 2. Of those that a mesh axis runs over, the one named last changes fastest.
Arguments:
- train_gate: float32 [64, 2048, 1024], P('ep', 'fsdp'), may hold values from -0.1875 to 0.1875
- other_gate: float32 [64, 2048, 1024], P('ep', 'fsdp'), may hold values from -0.125 to 0.125
- train_up: float32 [64, 2048, 1024], P('ep', 'fsdp'), may hold values from -0.1875 to 0.1875
- other_up: float32 [64, 2048, 1024], P('ep', 'fsdp'), may hold values from -0.125 to 0.125
- mix_share: float32 [64], P('ep'), may hold values from 0.2 to 0.8
- router_weight: float32 [2048, 64], P('fsdp', 'ep'), may hold values from -0.125 to 0.125
- router_gain: float32 [2048], P('fsdp'), may hold values from 0.25 to 1.75
Outputs:
- ready_gate: bfloat16 [64, 2048, 1024], P('ep')
- ready_up: bfloat16 [64, 2048, 1024], P('ep')
- scale_gate: float32 [64, 1024], P('ep')
- scale_up: float32 [64, 1024], P('ep')
- serve_router: bfloat16 [2048, 64], replicated
The draws below stay inside these ranges and needn't reach their ends.
All inputs are finite; a program needn't handle non-finite values. Where the reference program divides by a largest or mean magnitude, that divisor is 1e-20 or more.
Results may differ from the reference program's by a relative error of at most 0.001.
Values may be sent and summed in bfloat16 or wider, within the bound.
A program may use at most 64 MiB of HBM per device.

```python
import jax
import jax.numpy as jnp

EXPERTS = 64
D_MODEL = 2048
D_EXPERT = 1024


def with_spikes(drawn, stream_key, source, target, shards_of, factor):
    owner, partner = [(jnp.arange(drawn.shape[dim]) // (drawn.shape[dim] // shards_of)).reshape([-1 if axis == dim else 1 for axis in range(drawn.ndim)]) for dim in (source, target)]
    chosen = jax.random.permutation(stream_key, shards_of)[partner]
    strong = (owner == chosen) | (owner == (partner + shards_of // 2) % shards_of)
    return jnp.where(strong, factor * drawn, drawn)


def steps_of(key, dims, split, least, top_value):
    def one(position, shards_of):
        steps = jax.random.uniform(jax.random.fold_in(jax.random.fold_in(key, 6), position), (shards_of,), jnp.float32, least / len(split), top_value / len(split))
        return jnp.repeat(jnp.exp(steps), dims[position] // shards_of).reshape((-1,) + (1,) * (len(dims) - position - 1))

    gain = one(*split[0])
    for cut in split[1:]:
        gain = gain * one(*cut)
    return gain


def bell_draw(key, shape, spread, bound, pieces=(), dtype=jnp.bfloat16):
    result = jax.random.normal(key, shape, jnp.float32) * spread
    if len(pieces) > 0:
        result = steps_of(key, shape, pieces, -0.22, 0.18) * result
    return jnp.clip(result, min=-bound, max=bound).astype(dtype)


def bell_draw_with(stream_key, dims, width, reach, cuts, heavy, kind=jnp.bfloat16):
    drawn = width * jax.random.normal(stream_key, dims, jnp.float32)
    if cuts:
        drawn = drawn * steps_of(stream_key, dims, cuts, -0.22, 0.18)
    return jnp.clip(with_spikes(drawn, jax.random.fold_in(stream_key, 3), *heavy), -reach, reach).astype(kind)


def setup_inputs(seed: int = 0) -> dict:
    arg_keys = jax.random.split(jax.random.key(seed), 8)
    train_gate = bell_draw_with(arg_keys[0], (EXPERTS, D_MODEL, D_EXPERT), D_MODEL ** -0.5, 0.1875, ((0, 64), (1, 4)), (1, 2, 4, 2.0), jnp.float32)
    other_gate = bell_draw(arg_keys[1], (EXPERTS, D_MODEL, D_EXPERT), D_MODEL ** -0.5, 0.125, ((0, 64), (1, 4)), jnp.float32)
    train_up = bell_draw_with(arg_keys[2], (EXPERTS, D_MODEL, D_EXPERT), D_MODEL ** -0.5, 0.1875, ((0, 64), (1, 4)), (1, 2, 4, 2.0), jnp.float32)
    other_up = bell_draw(arg_keys[3], (EXPERTS, D_MODEL, D_EXPERT), D_MODEL ** -0.5, 0.125, ((0, 64), (1, 4)), jnp.float32)
    mix_share = jnp.clip(0.2 + 0.6 * jax.random.uniform(arg_keys[4], (EXPERTS,), jnp.float32) ** steps_of(arg_keys[4], (EXPERTS,), ((0, 64),), -0.2, 0.2), 0.2, 0.8)
    router_weight = bell_draw(arg_keys[5], (D_MODEL, EXPERTS), D_MODEL ** -0.5, 0.125, ((0, 4), (1, 64)), jnp.float32)
    router_gain = jnp.clip(1.0 + 0.15 * jax.random.normal(arg_keys[6], (D_MODEL,), jnp.float32), 0.25, 1.75)
    return dict(train_gate=train_gate, other_gate=other_gate, train_up=train_up, other_up=other_up, mix_share=mix_share, router_weight=router_weight, router_gain=router_gain)


def reference(train_gate, other_gate, train_up, other_up, mix_share, router_weight, router_gain):
    latest_gate = mix_share[:, None, None] * train_gate + (1.0 - mix_share[:, None, None]) * other_gate
    latest_up = mix_share[:, None, None] * train_up + (1.0 - mix_share[:, None, None]) * other_up
    scale_gate = jnp.max(jnp.abs(latest_gate), axis=1)
    ready_gate = (latest_gate / jnp.expand_dims(scale_gate, 1)).astype(jnp.bfloat16)
    scale_up = jnp.max(jnp.abs(latest_up), axis=1)
    ready_up = (latest_up / jnp.expand_dims(scale_up, 1)).astype(jnp.bfloat16)
    serve_router = (router_weight * router_gain[:, None]).astype(jnp.bfloat16)
    return ready_gate, ready_up, scale_gate, scale_up, serve_router
```

```python
import functools

import jax
import jax.numpy as jnp
from jax import lax
from jax.experimental import pallas as pl
from jax.experimental.pallas import tpu as pltpu
from jax.sharding import PartitionSpec as P

MESH = pl.DeviceIdType.MESH
X, Y, Z = 4, 4, 8
ROWS, COLS = 512, 1024
WIDTH = 256
PER = COLS // WIDTH
CHUNKS = 2 * PER
HALF = ROWS // 2
STEP = 64


def main_kernel(
    share, tg, og, tu, ou, rw, rg,
    out, sc, rout,
    tbuf, obuf, mx, rwv, rgv, rt, stage,
    ld_sem, small_sem, mx_send, mx_recv, own_send, own_recv, fwd_send, fwd_recv,
    r1_send, r1_recv, r2_send, r2_recv, r3_send, r3_recv, r4_send, r4_recv,
):
    x = lax.axis_index("fsdp")
    ep = lax.axis_index("ep")
    core = lax.rem(ep, 2)
    y = lax.rem(ep // 2, Y)
    z = ep // (2 * Y)

    right, left, opp = (lax.rem(x + k, X) for k in (1, X - 1, 2))
    x_peers = tuple({"fsdp": p} for p in (right, left, opp))
    at = lambda zz, yy, cc: {"ep": (zz * Y + yy) * 2 + cc}
    y_peers = tuple(at(z, lax.rem(y + k, Y), core) for k in (1, 2, 3))
    z_up, z_down = lax.rem(z + 1, Z), lax.rem(z + Z - 1, Z)
    z_peers = (at(z_up, y, core), at(z_down, y, core))
    partner = at(z, y, 1 - core)

    barrier = pltpu.get_barrier_semaphore()
    for peer in (*x_peers, *y_peers, *z_peers, partner):
        pl.semaphore_signal(barrier, inc=1, device_id=peer, device_id_type=MESH)

    def load(j, which):
        src = ((tg, og), (tu, ou))[j // PER][which]
        cols = pl.ds((j % PER) * WIDTH, WIDTH)
        return pltpu.make_async_copy(
            src.at[0, :, cols], (tbuf, obuf)[which].at[j], ld_sem.at[j, which]
        )

    small = (
        pltpu.make_async_copy(rw, rwv, small_sem.at[0]),
        pltpu.make_async_copy(rg, rgv, small_sem.at[1]),
    )
    for j in range(CHUNKS):
        load(j, 0).start()
        load(j, 1).start()
    for c in small:
        c.start()

    def max_copy(j, k):
        return pltpu.make_async_remote_copy(
            src_ref=mx.at[j, x], dst_ref=mx.at[j, x],
            send_sem=mx_send.at[j, k], recv_sem=mx_recv.at[j, k],
            device_id=x_peers[k], device_id_type=MESH,
        )

    def own_copy(j, d, h):
        piece = out.at[j, x, pl.ds(h * HALF, HALF)]
        return pltpu.make_async_remote_copy(
            src_ref=piece, dst_ref=piece,
            send_sem=own_send.at[j, d, h], recv_sem=own_recv.at[j, d, h],
            device_id=x_peers[d], device_id_type=MESH,
        )

    def forward_copy(j, d):
        source = (left, right)[d]
        piece = out.at[j, source, pl.ds(d * HALF, HALF)]
        return pltpu.make_async_remote_copy(
            src_ref=piece, dst_ref=piece,
            send_sem=fwd_send.at[j, d], recv_sem=fwd_recv.at[j, d],
            device_id=x_peers[d], device_id_type=MESH,
        )

    share_t = share[0]
    share_o = 1.0 - share_t

    for j in range(CHUNKS):
        load(j, 0).wait()
        load(j, 1).wait()

        def mix(i, top):
            rows = pl.ds(pl.multiple_of(i * STEP, STEP), STEP)
            latest = share_t * tbuf[j, rows, :] + share_o * obuf[j, rows, :]
            tbuf[j, rows, :] = latest
            return jnp.maximum(top, jnp.max(jnp.abs(latest).reshape(STEP // 8, 8, WIDTH), axis=0))

        top = lax.fori_loop(0, ROWS // STEP, mix, jnp.zeros((8, WIDTH), jnp.float32), unroll=True)
        mx[j, x] = jnp.max(top, axis=0, keepdims=True)
        if j == 0:
            pl.semaphore_wait(barrier, 9)
        for k in (2, 0, 1):
            max_copy(j, k).start()

    for j in range(CHUNKS):
        for k in range(3):
            max_copy(j, k).wait_recv()
        scale = jnp.maximum(
            jnp.maximum(mx[j, 0], mx[j, 1]), jnp.maximum(mx[j, 2], mx[j, 3])
        )
        sc[j] = scale

        def divide(i, carry):
            rows = pl.ds(pl.multiple_of(i * STEP, STEP), STEP)
            out[j, x, rows, :] = (tbuf[j, rows, :] / scale).astype(jnp.bfloat16)
            return carry

        lax.fori_loop(0, ROWS // STEP, divide, 0, unroll=True)
        for h in range(2):
            own_copy(j, 0, h).start()
            own_copy(j, 1, 1 - h).start()

    for c in small:
        c.wait()
    piece = rwv[...] * rgv[...]
    for r in range(4):
        rt[core, z, y, x, pl.ds(r, 1), :] = piece[:, r * 128 : (r + 1) * 128]

    def r1(k):
        ref = rt.at[core, z, y, x]
        return pltpu.make_async_remote_copy(
            src_ref=ref, dst_ref=ref, send_sem=r1_send.at[k], recv_sem=r1_recv.at[k],
            device_id=x_peers[k], device_id_type=MESH,
        )

    def r2(k):
        ref = rt.at[core, z, y]
        return pltpu.make_async_remote_copy(
            src_ref=ref, dst_ref=ref, send_sem=r2_send.at[k], recv_sem=r2_recv.at[k],
            device_id=y_peers[k], device_id_type=MESH,
        )

    def r3(k, d):
        source = lax.rem(z + (Z - k if d == 0 else k), Z)
        ref = rt.at[core, source]
        return pltpu.make_async_remote_copy(
            src_ref=ref, dst_ref=ref, send_sem=r3_send.at[k, d], recv_sem=r3_recv.at[k, d],
            device_id=z_peers[d], device_id_type=MESH,
        )

    r4 = pltpu.make_async_remote_copy(
        src_ref=rt.at[core], dst_ref=rt.at[core], send_sem=r4_send, recv_sem=r4_recv,
        device_id=partner, device_id_type=MESH,
    )
    for k in range(3):
        r1(k).start()
    for k in range(3):
        r1(k).wait_recv()
    for k in range(3):
        r2(k).start()
    for k in range(3):
        r2(k).wait_recv()
    for k in range(Z // 2):
        r3(k, 0).start()
        if k < Z // 2 - 1:
            r3(k, 1).start()
        r3(k, 0).wait_recv()
        if k < Z // 2 - 1:
            r3(k, 1).wait_recv()
    r4.start()
    r4.wait_recv()

    def spread(zz, carry):
        rows = pl.ds(pl.multiple_of(zz * 2 * Y, 2 * Y), 2 * Y)
        for xx in range(X):
            for r in range(4):
                stage[rows, (xx * 4 + r) * 128 : (xx * 4 + r + 1) * 128] = jnp.concatenate(
                    [rt[e % 2, zz, e // 2, xx, pl.ds(r, 1), :] for e in range(2 * Y)], axis=0
                )
        return carry

    lax.fori_loop(0, Z, spread, 0)

    def narrow(i, carry):
        rows = pl.ds(pl.multiple_of(i * 16, 16), 16)
        rout[rows, :] = stage[rows, :].astype(jnp.bfloat16)
        return carry

    lax.fori_loop(0, 4, narrow, 0)

    for j in range(CHUNKS):
        own_copy(j, 0, 0).wait_recv()
        forward_copy(j, 0).start()
        own_copy(j, 1, 1).wait_recv()
        forward_copy(j, 1).start()

    for j in range(CHUNKS):
        own_copy(j, 0, 1).wait_recv()
        own_copy(j, 1, 0).wait_recv()
        for d in range(2):
            for h in range(2):
                own_copy(j, d, h).wait_send()
        for k in range(3):
            max_copy(j, k).wait_send()
    for k in range(3):
        r1(k).wait_send()
        r2(k).wait_send()
    for k in range(Z // 2):
        r3(k, 0).wait_send()
        if k < Z // 2 - 1:
            r3(k, 1).wait_send()
    r4.wait_send()
    for j in range(CHUNKS):
        for d in range(2):
            forward_copy(j, d).wait_recv()
            forward_copy(j, d).wait_send()


def write_kernel(out, sc, rout, ready_gate, ready_up, scale_gate, scale_up, router, sem, sc_sem, r_sem):
    copies = []
    for j in range(CHUNKS):
        cols = pl.ds((j % PER) * WIDTH, WIDTH)
        for x in range(X):
            copies.append(
                pltpu.make_async_copy(
                    out.at[j, x],
                    (ready_gate, ready_up)[j // PER].at[0, pl.ds(x * ROWS, ROWS), cols],
                    sem.at[j, x],
                )
            )
        copies.append(
            pltpu.make_async_copy(
                sc.at[j], (scale_gate, scale_up)[j // PER].at[:, cols], sc_sem.at[j]
            )
        )
    copies.append(pltpu.make_async_copy(rout, router, r_sem))
    for c in copies:
        c.start()
    for c in copies:
        c.wait()


def per_device(train_gate, other_gate, train_up, other_up, mix_share, router_weight, router_gain):
    f32, bf16 = jnp.float32, jnp.bfloat16
    hbm = pl.BlockSpec(memory_space=pltpu.HBM)
    vmem = pl.BlockSpec(memory_space=pltpu.VMEM)
    dma = pltpu.SemaphoreType.DMA
    out, sc, rout = pl.pallas_call(
        main_kernel,
        out_shape=(
            pltpu.VMEM((CHUNKS, X, ROWS, WIDTH), bf16),
            pltpu.VMEM((CHUNKS, 1, WIDTH), f32),
            pltpu.VMEM((2 * Y * Z, X * ROWS), bf16),
        ),
        in_specs=[pl.BlockSpec(memory_space=pltpu.SMEM)] + [hbm] * 6,
        out_specs=(vmem, vmem, vmem),
        scratch_shapes=[
            pltpu.VMEM((CHUNKS, ROWS, WIDTH), f32),
            pltpu.VMEM((CHUNKS, ROWS, WIDTH), f32),
            pltpu.VMEM((CHUNKS, X, 1, WIDTH), f32),
            pltpu.VMEM((1, ROWS), f32),
            pltpu.VMEM((1, ROWS), f32),
            pltpu.VMEM((2, Z, Y, X, 4, 128), f32),
            pltpu.VMEM((2 * Y * Z, X * ROWS), f32),
            dma((CHUNKS, 2)), dma((2,)),
            dma((CHUNKS, 3)), dma((CHUNKS, 3)),
            dma((CHUNKS, 2, 2)), dma((CHUNKS, 2, 2)),
            dma((CHUNKS, 2)), dma((CHUNKS, 2)),
            dma((3,)), dma((3,)), dma((3,)), dma((3,)),
            dma((Z // 2, 2)), dma((Z // 2, 2)),
            dma, dma,
        ],
        compiler_params=pltpu.CompilerParams(
            collective_id=0, has_side_effects=True, vmem_limit_bytes=40 * 1024 * 1024
        ),
        name="gather",
    )(
        mix_share,
        *(
            pltpu.with_memory_space_constraint(a, pltpu.HBM)
            for a in (
                train_gate, other_gate, train_up, other_up,
                router_weight.reshape(1, ROWS), router_gain.reshape(1, ROWS),
            )
        )
    )
    ready_gate, ready_up, scale_gate, scale_up, router = pl.pallas_call(
        write_kernel,
        out_shape=(
            jax.ShapeDtypeStruct((1, X * ROWS, COLS), bf16),
            jax.ShapeDtypeStruct((1, X * ROWS, COLS), bf16),
            jax.ShapeDtypeStruct((1, COLS), f32),
            jax.ShapeDtypeStruct((1, COLS), f32),
            jax.ShapeDtypeStruct((2 * Y * Z, X * ROWS), bf16),
        ),
        in_specs=[vmem] * 3,
        out_specs=(hbm,) * 5,
        scratch_shapes=[dma((CHUNKS, X)), dma((CHUNKS,)), dma],
        compiler_params=pltpu.CompilerParams(vmem_limit_bytes=1024 * 1024),
        name="write",
    )(*(pltpu.with_memory_space_constraint(a, pltpu.VMEM) for a in (out, sc, rout)))
    return ready_gate, ready_up, scale_gate, scale_up, router.T


def solution(mesh):
    placed = (
        P("ep", "fsdp", None),
        P("ep", "fsdp", None),
        P("ep", "fsdp", None),
        P("ep", "fsdp", None),
        P("ep"),
        P("fsdp", "ep"),
        P("fsdp"),
    )
    return jax.shard_map(
        per_device,
        mesh=mesh,
        in_specs=placed,
        out_specs=(P("ep", None, None), P("ep", None, None), P("ep", None), P("ep", None), P()),
        check_vma=False,
    )
```

```python
import functools

import jax
import jax.numpy as jnp
from jax import lax
from jax.experimental import pallas as pl
from jax.experimental.pallas import tpu as pltpu
from jax.sharding import PartitionSpec as P

MESH = pl.DeviceIdType.MESH
X, Y, Z = 4, 4, 8
ROWS, COLS = 512, 1024
WIDTH = 256
PER = COLS // WIDTH
CHUNKS = 2 * PER
HALF = ROWS // 2
STEP = 64


def main_kernel(
    share, tg, og, tu, ou, rw, rg,
    out, sc, rout,
    tbuf, obuf, mx, rwv, rgv, rt, stage,
    ld_sem, small_sem, mx_send, mx_recv, own_send, own_recv, fwd_send, fwd_recv,
    r1_send, r1_recv, r2_send, r2_recv, r3_send, r3_recv, r4_send, r4_recv,
):
    x = lax.axis_index("fsdp")
    ep = lax.axis_index("ep")
    core = lax.rem(ep, 2)
    y = lax.rem(ep // 2, Y)
    z = ep // (2 * Y)

    right, left, opp = (lax.rem(x + k, X) for k in (1, X - 1, 2))
    x_peers = tuple({"fsdp": p} for p in (right, left, opp))
    at = lambda zz, yy, cc: {"ep": (zz * Y + yy) * 2 + cc}
    y_peers = tuple(at(z, lax.rem(y + k, Y), core) for k in (1, 2, 3))
    z_up, z_down = lax.rem(z + 1, Z), lax.rem(z + Z - 1, Z)
    z_peers = (at(z_up, y, core), at(z_down, y, core))
    partner = at(z, y, 1 - core)

    barrier = pltpu.get_barrier_semaphore()
    for peer in (*x_peers, *y_peers, *z_peers, partner):
        pl.semaphore_signal(barrier, inc=1, device_id=peer, device_id_type=MESH)

    def load(j, which):
        src = ((tg, og), (tu, ou))[j // PER][which]
        cols = pl.ds((j % PER) * WIDTH, WIDTH)
        return pltpu.make_async_copy(
            src.at[0, :, cols], (tbuf, obuf)[which].at[j], ld_sem.at[j, which]
        )

    small = (
        pltpu.make_async_copy(rw, rwv, small_sem.at[0]),
        pltpu.make_async_copy(rg, rgv, small_sem.at[1]),
    )
    for j in range(CHUNKS):
        load(j, 0).start()
        load(j, 1).start()
        if j == 0:
            for c in small:
                c.start()

    def max_copy(j, k):
        return pltpu.make_async_remote_copy(
            src_ref=mx.at[j, x], dst_ref=mx.at[j, x],
            send_sem=mx_send.at[j, k], recv_sem=mx_recv.at[j, k],
            device_id=x_peers[k], device_id_type=MESH,
        )

    def own_copy(j, d, h):
        piece = out.at[j, x, pl.ds(h * HALF, HALF)]
        return pltpu.make_async_remote_copy(
            src_ref=piece, dst_ref=piece,
            send_sem=own_send.at[j, d, h], recv_sem=own_recv.at[j, d, h],
            device_id=x_peers[d], device_id_type=MESH,
        )

    def forward_copy(j, d):
        source = (left, right)[d]
        piece = out.at[j, source, pl.ds(d * HALF, HALF)]
        return pltpu.make_async_remote_copy(
            src_ref=piece, dst_ref=piece,
            send_sem=fwd_send.at[j, d], recv_sem=fwd_recv.at[j, d],
            device_id=x_peers[d], device_id_type=MESH,
        )

    def r1(k):
        ref = rt.at[core, z, y, x]
        return pltpu.make_async_remote_copy(
            src_ref=ref, dst_ref=ref, send_sem=r1_send.at[k], recv_sem=r1_recv.at[k],
            device_id=x_peers[k], device_id_type=MESH,
        )

    def r2(k):
        ref = rt.at[core, z, y]
        return pltpu.make_async_remote_copy(
            src_ref=ref, dst_ref=ref, send_sem=r2_send.at[k], recv_sem=r2_recv.at[k],
            device_id=y_peers[k], device_id_type=MESH,
        )

    def r3(k, d):
        source = lax.rem(z + (Z - k if d == 0 else k), Z)
        ref = rt.at[core, source]
        return pltpu.make_async_remote_copy(
            src_ref=ref, dst_ref=ref, send_sem=r3_send.at[k, d], recv_sem=r3_recv.at[k, d],
            device_id=z_peers[d], device_id_type=MESH,
        )

    r4 = pltpu.make_async_remote_copy(
        src_ref=rt.at[core], dst_ref=rt.at[core], send_sem=r4_send, recv_sem=r4_recv,
        device_id=partner, device_id_type=MESH,
    )
    share_t = share[0]
    share_o = 1.0 - share_t

    for j in range(CHUNKS):
        load(j, 0).wait()
        load(j, 1).wait()

        def mix(i, top):
            rows = pl.ds(pl.multiple_of(i * STEP, STEP), STEP)
            latest = share_t * tbuf[j, rows, :] + share_o * obuf[j, rows, :]
            tbuf[j, rows, :] = latest
            return jnp.maximum(top, jnp.max(jnp.abs(latest).reshape(STEP // 8, 8, WIDTH), axis=0))

        top = lax.fori_loop(0, ROWS // STEP, mix, jnp.zeros((8, WIDTH), jnp.float32), unroll=True)
        mx[j, x] = jnp.max(top, axis=0, keepdims=True)
        if j == 0:
            pl.semaphore_wait(barrier, 9)
        for k in (2, 0, 1):
            max_copy(j, k).start()
        if j == 0:
            for c in small:
                c.wait()
            piece = rwv[...] * rgv[...]
            for r in range(4):
                rt[core, z, y, x, pl.ds(r, 1), :] = piece[:, r * 128 : (r + 1) * 128]
            for k in (2, 0, 1):
                r1(k).start()

    for j in range(CHUNKS):
        for k in range(3):
            max_copy(j, k).wait_recv()
        scale = jnp.maximum(
            jnp.maximum(mx[j, 0], mx[j, 1]), jnp.maximum(mx[j, 2], mx[j, 3])
        )
        sc[j] = scale

        def divide(i, carry):
            rows = pl.ds(pl.multiple_of(i * STEP, STEP), STEP)
            out[j, x, rows, :] = (tbuf[j, rows, :] / scale).astype(jnp.bfloat16)
            return carry

        lax.fori_loop(0, ROWS // STEP, divide, 0, unroll=True)
        for h in range(2):
            own_copy(j, 0, h).start()
            own_copy(j, 1, 1 - h).start()

    for k in range(3):
        r1(k).wait_recv()
    for k in range(3):
        r2(k).start()
    for k in range(3):
        r2(k).wait_recv()
    for k in range(Z // 2):
        r3(k, 0).start()
        if k < Z // 2 - 1:
            r3(k, 1).start()
        r3(k, 0).wait_recv()
        if k < Z // 2 - 1:
            r3(k, 1).wait_recv()
    r4.start()
    r4.wait_recv()

    def spread(zz, carry):
        rows = pl.ds(pl.multiple_of(zz * 2 * Y, 2 * Y), 2 * Y)
        for xx in range(X):
            for r in range(4):
                stage[rows, (xx * 4 + r) * 128 : (xx * 4 + r + 1) * 128] = jnp.concatenate(
                    [rt[e % 2, zz, e // 2, xx, pl.ds(r, 1), :] for e in range(2 * Y)], axis=0
                )
        return carry

    lax.fori_loop(0, Z, spread, 0)

    def narrow(i, carry):
        rows = pl.ds(pl.multiple_of(i * 16, 16), 16)
        rout[rows, :] = stage[rows, :].astype(jnp.bfloat16)
        return carry

    lax.fori_loop(0, 4, narrow, 0)

    for j in range(CHUNKS):
        own_copy(j, 0, 0).wait_recv()
        forward_copy(j, 0).start()
        own_copy(j, 1, 1).wait_recv()
        forward_copy(j, 1).start()

    for j in range(CHUNKS):
        own_copy(j, 0, 1).wait_recv()
        own_copy(j, 1, 0).wait_recv()
        for d in range(2):
            for h in range(2):
                own_copy(j, d, h).wait_send()
        for k in range(3):
            max_copy(j, k).wait_send()
    for k in range(3):
        r1(k).wait_send()
        r2(k).wait_send()
    for k in range(Z // 2):
        r3(k, 0).wait_send()
        if k < Z // 2 - 1:
            r3(k, 1).wait_send()
    r4.wait_send()
    for j in range(CHUNKS):
        for d in range(2):
            forward_copy(j, d).wait_recv()
            forward_copy(j, d).wait_send()


def write_kernel(out, sc, rout, ready_gate, ready_up, scale_gate, scale_up, router, sem, sc_sem, r_sem):
    copies = []
    for j in range(CHUNKS):
        cols = pl.ds((j % PER) * WIDTH, WIDTH)
        for x in range(X):
            copies.append(
                pltpu.make_async_copy(
                    out.at[j, x],
                    (ready_gate, ready_up)[j // PER].at[0, pl.ds(x * ROWS, ROWS), cols],
                    sem.at[j, x],
                )
            )
        copies.append(
            pltpu.make_async_copy(
                sc.at[j], (scale_gate, scale_up)[j // PER].at[:, cols], sc_sem.at[j]
            )
        )
    copies.append(pltpu.make_async_copy(rout, router, r_sem))
    for c in copies:
        c.start()
    for c in copies:
        c.wait()


def per_device(train_gate, other_gate, train_up, other_up, mix_share, router_weight, router_gain):
    f32, bf16 = jnp.float32, jnp.bfloat16
    hbm = pl.BlockSpec(memory_space=pltpu.HBM)
    vmem = pl.BlockSpec(memory_space=pltpu.VMEM)
    dma = pltpu.SemaphoreType.DMA
    out, sc, rout = pl.pallas_call(
        main_kernel,
        out_shape=(
            pltpu.VMEM((CHUNKS, X, ROWS, WIDTH), bf16),
            pltpu.VMEM((CHUNKS, 1, WIDTH), f32),
            pltpu.VMEM((2 * Y * Z, X * ROWS), bf16),
        ),
        in_specs=[pl.BlockSpec(memory_space=pltpu.SMEM)] + [hbm] * 6,
        out_specs=(vmem, vmem, vmem),
        scratch_shapes=[
            pltpu.VMEM((CHUNKS, ROWS, WIDTH), f32),
            pltpu.VMEM((CHUNKS, ROWS, WIDTH), f32),
            pltpu.VMEM((CHUNKS, X, 1, WIDTH), f32),
            pltpu.VMEM((1, ROWS), f32),
            pltpu.VMEM((1, ROWS), f32),
            pltpu.VMEM((2, Z, Y, X, 4, 128), f32),
            pltpu.VMEM((2 * Y * Z, X * ROWS), f32),
            dma((CHUNKS, 2)), dma((2,)),
            dma((CHUNKS, 3)), dma((CHUNKS, 3)),
            dma((CHUNKS, 2, 2)), dma((CHUNKS, 2, 2)),
            dma((CHUNKS, 2)), dma((CHUNKS, 2)),
            dma((3,)), dma((3,)), dma((3,)), dma((3,)),
            dma((Z // 2, 2)), dma((Z // 2, 2)),
            dma, dma,
        ],
        compiler_params=pltpu.CompilerParams(
            collective_id=0, has_side_effects=True, vmem_limit_bytes=40 * 1024 * 1024
        ),
        name="gather",
    )(
        mix_share,
        *(
            pltpu.with_memory_space_constraint(a, pltpu.HBM)
            for a in (
                train_gate, other_gate, train_up, other_up,
                router_weight.reshape(1, ROWS), router_gain.reshape(1, ROWS),
            )
        )
    )
    ready_gate, ready_up, scale_gate, scale_up, router = pl.pallas_call(
        write_kernel,
        out_shape=(
            jax.ShapeDtypeStruct((1, X * ROWS, COLS), bf16),
            jax.ShapeDtypeStruct((1, X * ROWS, COLS), bf16),
            jax.ShapeDtypeStruct((1, COLS), f32),
            jax.ShapeDtypeStruct((1, COLS), f32),
            jax.ShapeDtypeStruct((2 * Y * Z, X * ROWS), bf16),
        ),
        in_specs=[vmem] * 3,
        out_specs=(hbm,) * 5,
        scratch_shapes=[dma((CHUNKS, X)), dma((CHUNKS,)), dma],
        compiler_params=pltpu.CompilerParams(vmem_limit_bytes=1024 * 1024),
        name="write",
    )(*(pltpu.with_memory_space_constraint(a, pltpu.VMEM) for a in (out, sc, rout)))
    return ready_gate, ready_up, scale_gate, scale_up, router.T


def solution(mesh):
    placed = (
        P("ep", "fsdp", None),
        P("ep", "fsdp", None),
        P("ep", "fsdp", None),
        P("ep", "fsdp", None),
        P("ep"),
        P("fsdp", "ep"),
        P("fsdp"),
    )
    return jax.shard_map(
        per_device,
        mesh=mesh,
        in_specs=placed,
        out_specs=(P("ep", None, None), P("ep", None, None), P("ep", None), P("ep", None), P()),
        check_vma=False,
    )
```

```python
import functools

import jax
import jax.numpy as jnp
from jax import lax
from jax.experimental import pallas as pl
from jax.experimental.pallas import tpu as pltpu
from jax.sharding import PartitionSpec as P

MESH = pl.DeviceIdType.MESH
X, Y, Z = 4, 4, 8
ROWS, COLS = 512, 1024
WIDTH = 256
PER = COLS // WIDTH
CHUNKS = 2 * PER
HALF = ROWS // 2
STEP = 64


def main_kernel(
    share, tg, og, tu, ou, rw, rg,
    out, sc, rout,
    tbuf, obuf, mx, rwv, rgv, rt, stage,
    ld_sem, small_sem, mx_send, mx_recv, own_send, own_recv, fwd_send, fwd_recv,
    r1_send, r1_recv, r2_send, r2_recv, r3_send, r3_recv, r4_send, r4_recv,
):
    x = lax.axis_index("fsdp")
    ep = lax.axis_index("ep")
    core = lax.rem(ep, 2)
    y = lax.rem(ep // 2, Y)
    z = ep // (2 * Y)

    right, left, opp = (lax.rem(x + k, X) for k in (1, X - 1, 2))
    x_peers = tuple({"fsdp": p} for p in (right, left, opp))
    at = lambda zz, yy, cc: {"ep": (zz * Y + yy) * 2 + cc}
    y_up, y_down = at(z, lax.rem(y + 1, Y), core), at(z, lax.rem(y + Y - 1, Y), core)
    z_up, z_down = at(lax.rem(z + 1, Z), y, core), at(lax.rem(z + Z - 1, Z), y, core)
    partner = at(z, y, 1 - core)

    barrier = pltpu.get_barrier_semaphore()

    def greet(peer):
        pl.semaphore_signal(barrier, inc=1, device_id=peer, device_id_type=MESH)

    for peer in x_peers:
        greet(peer)
    pl.when(z < Z - 1)(lambda: greet(z_up))
    pl.when(y < Y - 1)(lambda: greet(y_up))
    pl.when(core == 0)(lambda: greet(partner))
    greeted = 3 + jnp.minimum(z, 1) + jnp.minimum(y, 1) + core

    def load(j, which):
        src = ((tg, og), (tu, ou))[j // PER][which]
        cols = pl.ds((j % PER) * WIDTH, WIDTH)
        return pltpu.make_async_copy(
            src.at[0, :, cols], (tbuf, obuf)[which].at[j], ld_sem.at[j, which]
        )

    small = (
        pltpu.make_async_copy(rw, rwv, small_sem.at[0]),
        pltpu.make_async_copy(rg, rgv, small_sem.at[1]),
    )
    def start_loads(j):
        load(j, 0).start()
        load(j, 1).start()

    def max_copy(j, k):
        return pltpu.make_async_remote_copy(
            src_ref=mx.at[j, x], dst_ref=mx.at[j, x],
            send_sem=mx_send.at[j, k], recv_sem=mx_recv.at[j, k],
            device_id=x_peers[k], device_id_type=MESH,
        )

    def own_copy(j, d, h):
        piece = out.at[j, x, pl.ds(h * HALF, HALF)]
        return pltpu.make_async_remote_copy(
            src_ref=piece, dst_ref=piece,
            send_sem=own_send.at[j, d, h], recv_sem=own_recv.at[j, d, h],
            device_id=x_peers[d], device_id_type=MESH,
        )

    def forward_copy(j, d):
        source = (left, right)[d]
        piece = out.at[j, source, pl.ds(d * HALF, HALF)]
        return pltpu.make_async_remote_copy(
            src_ref=piece, dst_ref=piece,
            send_sem=fwd_send.at[j, d], recv_sem=fwd_recv.at[j, d],
            device_id=x_peers[d], device_id_type=MESH,
        )

    def r1(k):
        ref = rt.at[core, z, y, x]
        return pltpu.make_async_remote_copy(
            src_ref=ref, dst_ref=ref, send_sem=r1_send.at[k], recv_sem=r1_recv.at[k],
            device_id=x_peers[k], device_id_type=MESH,
        )

    def line_copy(ref, peer, send_sem, recv_sem):
        return pltpu.make_async_remote_copy(
            src_ref=ref, dst_ref=ref, send_sem=send_sem, recv_sem=recv_sem,
            device_id=peer, device_id_type=MESH,
        )

    def along(pos, n, block, up_peer, down_peer, send, recv):
        down = lambda k: line_copy(
            block(lax.rem(pos + k, n)), down_peer, send.at[k, 0], recv.at[k, 0]
        )
        up = lambda k: line_copy(
            block(lax.rem(pos + n - k, n)), up_peer, send.at[k, 1], recv.at[k, 1]
        )
        sends_down = lambda k: (pos >= 1) & (pos + k <= n - 1)
        sends_up = lambda k: (pos <= n - 2) & (pos >= k)
        gets_down = lambda k: pos + 1 + k <= n - 1
        gets_up = lambda k: pos >= 1 + k

        def run():
            pl.when(sends_down(0))(lambda: down(0).start())
            for k in range(n - 1):
                pl.when(gets_down(k))(lambda: down(k).wait_recv())
                if k + 1 < n - 1:
                    pl.when(sends_down(k + 1))(lambda: down(k + 1).start())
                if k > 0:
                    pl.when(gets_up(k - 1))(lambda: up(k - 1).wait_recv())
                pl.when(sends_up(k))(lambda: up(k).start())
            pl.when(gets_up(n - 2))(lambda: up(n - 2).wait_recv())

        def drain():
            for k in range(n - 1):
                pl.when(sends_down(k))(lambda: down(k).wait_send())
                pl.when(sends_up(k))(lambda: up(k).wait_send())

        return run, drain

    run_y, drain_y = along(
        y, Y, lambda i: rt.at[core, z, i], y_up, y_down, r2_send, r2_recv
    )
    run_z, drain_z = along(
        z, Z, lambda i: rt.at[core, i], z_up, z_down, r3_send, r3_recv
    )

    r4 = pltpu.make_async_remote_copy(
        src_ref=rt.at[core], dst_ref=rt.at[core], send_sem=r4_send, recv_sem=r4_recv,
        device_id=partner, device_id_type=MESH,
    )
    share_t = share[0]
    share_o = 1.0 - share_t

    def local(j):
        load(j, 0).wait()
        load(j, 1).wait()

        def mix(i, top):
            rows = pl.ds(pl.multiple_of(i * STEP, STEP), STEP)
            latest = share_t * tbuf[j, rows, :] + share_o * obuf[j, rows, :]
            tbuf[j, rows, :] = latest
            return jnp.maximum(top, jnp.max(jnp.abs(latest).reshape(STEP // 8, 8, WIDTH), axis=0))

        top = lax.fori_loop(0, ROWS // STEP, mix, jnp.zeros((8, WIDTH), jnp.float32), unroll=True)
        mx[j, x] = jnp.max(top, axis=0, keepdims=True)

    def finish(j):
        for k in range(3):
            max_copy(j, k).wait_recv()
        scale = jnp.maximum(
            jnp.maximum(mx[j, 0], mx[j, 1]), jnp.maximum(mx[j, 2], mx[j, 3])
        )
        sc[j] = scale

        def divide(i, carry):
            rows = pl.ds(pl.multiple_of(i * STEP, STEP), STEP)
            out[j, x, rows, :] = (tbuf[j, rows, :] / scale).astype(jnp.bfloat16)
            return carry

        for h in range(2):
            lax.fori_loop(h * (HALF // STEP), (h + 1) * (HALF // STEP), divide, 0, unroll=True)
            own_copy(j, 0, h).start()
            own_copy(j, 1, h).start()

    start_loads(0)
    for c in small:
        c.start()
    for j in range(1, CHUNKS):
        start_loads(j)
    for j in range(CHUNKS):
        local(j)
        if j == 0:
            pl.semaphore_wait(barrier, greeted)
        for k in (2, 0, 1):
            max_copy(j, k).start()
        if j == 0:
            for c in small:
                c.wait()
            piece = rwv[...] * rgv[...]
            for r in range(4):
                rt[core, z, y, x, pl.ds(r, 1), :] = piece[:, r * 128 : (r + 1) * 128]
            for k in (2, 0, 1):
                r1(k).start()
        if j == 3:
            finish(0)
    for j in range(1, CHUNKS):
        finish(j)

    for k in range(3):
        r1(k).wait_recv()
    run_y()
    run_z()
    for j in range(CHUNKS):
        own_copy(j, 0, 0).wait_recv()
        forward_copy(j, 0).start()
        own_copy(j, 1, 1).wait_recv()
        forward_copy(j, 1).start()

    pl.when(core == 1)(lambda: r4.start())
    r4.wait_recv()
    pl.when(core == 0)(lambda: r4.start())

    def spread(zz, carry):
        rows = pl.ds(pl.multiple_of(zz * 2 * Y, 2 * Y), 2 * Y)
        for xx in range(X):
            for r in range(4):
                stage[rows, (xx * 4 + r) * 128 : (xx * 4 + r + 1) * 128] = jnp.concatenate(
                    [rt[e % 2, zz, e // 2, xx, pl.ds(r, 1), :] for e in range(2 * Y)], axis=0
                )
        return carry

    lax.fori_loop(0, Z, spread, 0)

    def narrow(i, carry):
        rows = pl.ds(pl.multiple_of(i * 16, 16), 16)
        rout[rows, :] = stage[rows, :].astype(jnp.bfloat16)
        return carry

    lax.fori_loop(0, 4, narrow, 0)

    for j in range(CHUNKS):
        own_copy(j, 0, 1).wait_recv()
        own_copy(j, 1, 0).wait_recv()
        for d in range(2):
            for h in range(2):
                own_copy(j, d, h).wait_send()
        for k in range(3):
            max_copy(j, k).wait_send()
    for k in range(3):
        r1(k).wait_send()
    drain_y()
    drain_z()
    r4.wait_send()
    for j in range(CHUNKS):
        for d in range(2):
            forward_copy(j, d).wait_recv()
            forward_copy(j, d).wait_send()


def write_kernel(out, sc, rout, ready_gate, ready_up, scale_gate, scale_up, router, sem, sc_sem, r_sem):
    copies = []
    for j in range(CHUNKS):
        cols = pl.ds((j % PER) * WIDTH, WIDTH)
        for x in range(X):
            copies.append(
                pltpu.make_async_copy(
                    out.at[j, x],
                    (ready_gate, ready_up)[j // PER].at[0, pl.ds(x * ROWS, ROWS), cols],
                    sem.at[j, x],
                )
            )
        copies.append(
            pltpu.make_async_copy(
                sc.at[j], (scale_gate, scale_up)[j // PER].at[:, cols], sc_sem.at[j]
            )
        )
    copies.append(pltpu.make_async_copy(rout, router, r_sem))
    for c in copies:
        c.start()
    for c in copies:
        c.wait()


def per_device(train_gate, other_gate, train_up, other_up, mix_share, router_weight, router_gain):
    f32, bf16 = jnp.float32, jnp.bfloat16
    hbm = pl.BlockSpec(memory_space=pltpu.HBM)
    vmem = pl.BlockSpec(memory_space=pltpu.VMEM)
    dma = pltpu.SemaphoreType.DMA
    out, sc, rout = pl.pallas_call(
        main_kernel,
        out_shape=(
            pltpu.VMEM((CHUNKS, X, ROWS, WIDTH), bf16),
            pltpu.VMEM((CHUNKS, 1, WIDTH), f32),
            pltpu.VMEM((2 * Y * Z, X * ROWS), bf16),
        ),
        in_specs=[pl.BlockSpec(memory_space=pltpu.SMEM)] + [hbm] * 6,
        out_specs=(vmem, vmem, vmem),
        scratch_shapes=[
            pltpu.VMEM((CHUNKS, ROWS, WIDTH), f32),
            pltpu.VMEM((CHUNKS, ROWS, WIDTH), f32),
            pltpu.VMEM((CHUNKS, X, 1, WIDTH), f32),
            pltpu.VMEM((1, ROWS), f32),
            pltpu.VMEM((1, ROWS), f32),
            pltpu.VMEM((2, Z, Y, X, 4, 128), f32),
            pltpu.VMEM((2 * Y * Z, X * ROWS), f32),
            dma((CHUNKS, 2)), dma((2,)),
            dma((CHUNKS, 3)), dma((CHUNKS, 3)),
            dma((CHUNKS, 2, 2)), dma((CHUNKS, 2, 2)),
            dma((CHUNKS, 2)), dma((CHUNKS, 2)),
            dma((3,)), dma((3,)), dma((Y - 1, 2)), dma((Y - 1, 2)),
            dma((Z - 1, 2)), dma((Z - 1, 2)),
            dma, dma,
        ],
        compiler_params=pltpu.CompilerParams(
            collective_id=0, has_side_effects=True, vmem_limit_bytes=40 * 1024 * 1024
        ),
        name="gather",
    )(
        mix_share,
        *(
            pltpu.with_memory_space_constraint(a, pltpu.HBM)
            for a in (
                train_gate, other_gate, train_up, other_up,
                router_weight.reshape(1, ROWS), router_gain.reshape(1, ROWS),
            )
        )
    )
    ready_gate, ready_up, scale_gate, scale_up, router = pl.pallas_call(
        write_kernel,
        out_shape=(
            jax.ShapeDtypeStruct((1, X * ROWS, COLS), bf16),
            jax.ShapeDtypeStruct((1, X * ROWS, COLS), bf16),
            jax.ShapeDtypeStruct((1, COLS), f32),
            jax.ShapeDtypeStruct((1, COLS), f32),
            jax.ShapeDtypeStruct((2 * Y * Z, X * ROWS), bf16),
        ),
        in_specs=[vmem] * 3,
        out_specs=(hbm,) * 5,
        scratch_shapes=[dma((CHUNKS, X)), dma((CHUNKS,)), dma],
        compiler_params=pltpu.CompilerParams(vmem_limit_bytes=1024 * 1024),
        name="write",
    )(*(pltpu.with_memory_space_constraint(a, pltpu.VMEM) for a in (out, sc, rout)))
    return ready_gate, ready_up, scale_gate, scale_up, router.T


def solution(mesh):
    placed = (
        P("ep", "fsdp", None),
        P("ep", "fsdp", None),
        P("ep", "fsdp", None),
        P("ep", "fsdp", None),
        P("ep"),
        P("fsdp", "ep"),
        P("fsdp"),
    )
    return jax.shard_map(
        per_device,
        mesh=mesh,
        in_specs=placed,
        out_specs=(P("ep", None, None), P("ep", None, None), P("ep", None), P("ep", None), P()),
        check_vma=False,
    )
```

```python
import functools

import jax
import jax.numpy as jnp
from jax import lax
from jax.experimental import pallas as pl
from jax.experimental.pallas import tpu as pltpu
from jax.sharding import PartitionSpec as P

MESH = pl.DeviceIdType.MESH
X, Y, Z = 4, 4, 8
ROWS, COLS = 512, 1024
WIDTH = 256
PER = COLS // WIDTH
CHUNKS = 2 * PER
OWN = (((0, 1), (1, 3), (4, 4)), ((0, 1), (4, 4), (1, 3)))
ONWARD = (((0, 4), (0, 1)), ((4, 4), (1,)))
STEP = 64


def main_kernel(
    share, tg, og, tu, ou, rw, rg,
    out, sc, rout,
    tbuf, obuf, mx, rwv, rgv, rt, stage,
    ld_sem, small_sem, mx_send, mx_recv, own_send, own_recv, fwd_send, fwd_recv,
    r1_send, r1_recv, r2_send, r2_recv, r3_send, r3_recv, r4_send, r4_recv,
):
    x = lax.axis_index("fsdp")
    ep = lax.axis_index("ep")
    core = lax.rem(ep, 2)
    y = lax.rem(ep // 2, Y)
    z = ep // (2 * Y)

    right, left, opp = (lax.rem(x + k, X) for k in (1, X - 1, 2))
    x_peers = tuple({"fsdp": p} for p in (right, left, opp))
    at = lambda zz, yy, cc: {"ep": (zz * Y + yy) * 2 + cc}
    y_up, y_down = at(z, lax.rem(y + 1, Y), core), at(z, lax.rem(y + Y - 1, Y), core)
    z_up, z_down = at(lax.rem(z + 1, Z), y, core), at(lax.rem(z + Z - 1, Z), y, core)
    partner = at(z, y, 1 - core)

    barrier = pltpu.get_barrier_semaphore()

    def greet(peer):
        pl.semaphore_signal(barrier, inc=1, device_id=peer, device_id_type=MESH)

    for peer in x_peers:
        greet(peer)
    pl.when(z < Z - 1)(lambda: greet(z_up))
    pl.when(y < Y - 1)(lambda: greet(y_up))
    pl.when(core == 0)(lambda: greet(partner))
    greeted = 3 + jnp.minimum(z, 1) + jnp.minimum(y, 1) + core

    def load(j, which):
        src = ((tg, og), (tu, ou))[j // PER][which]
        cols = pl.ds((j % PER) * WIDTH, WIDTH)
        return pltpu.make_async_copy(
            src.at[0, :, cols], (tbuf, obuf)[which].at[j], ld_sem.at[j, which]
        )

    small = (
        pltpu.make_async_copy(rw, rwv, small_sem.at[0]),
        pltpu.make_async_copy(rg, rgv, small_sem.at[1]),
    )
    def start_loads(j):
        load(j, 0).start()
        load(j, 1).start()

    def max_copy(j, k):
        return pltpu.make_async_remote_copy(
            src_ref=mx.at[j, x], dst_ref=mx.at[j, x],
            send_sem=mx_send.at[j, k], recv_sem=mx_recv.at[j, k],
            device_id=x_peers[k], device_id_type=MESH,
        )

    def block(chunks, device):
        first, number = chunks
        return out.at[pl.ds(first, number), pl.ds(pl.multiple_of(device * ROWS, ROWS), ROWS)]

    def own_copy(d, i):
        piece = block(OWN[d][i], x)
        return pltpu.make_async_remote_copy(
            src_ref=piece, dst_ref=piece,
            send_sem=own_send.at[d, i], recv_sem=own_recv.at[d, i],
            device_id=x_peers[d], device_id_type=MESH,
        )

    def forward_copy(d):
        piece = block(ONWARD[d][0], (left, right)[d])
        return pltpu.make_async_remote_copy(
            src_ref=piece, dst_ref=piece,
            send_sem=fwd_send.at[d], recv_sem=fwd_recv.at[d],
            device_id=x_peers[d], device_id_type=MESH,
        )

    def r1(k):
        ref = rt.at[core, z, y, x]
        return pltpu.make_async_remote_copy(
            src_ref=ref, dst_ref=ref, send_sem=r1_send.at[k], recv_sem=r1_recv.at[k],
            device_id=x_peers[k], device_id_type=MESH,
        )

    def line_copy(ref, peer, send_sem, recv_sem):
        return pltpu.make_async_remote_copy(
            src_ref=ref, dst_ref=ref, send_sem=send_sem, recv_sem=recv_sem,
            device_id=peer, device_id_type=MESH,
        )

    def along(pos, n, block, up_peer, down_peer, send, recv):
        down = lambda k: line_copy(
            block(lax.rem(pos + k, n)), down_peer, send.at[k, 0], recv.at[k, 0]
        )
        up = lambda k: line_copy(
            block(lax.rem(pos + n - k, n)), up_peer, send.at[k, 1], recv.at[k, 1]
        )
        sends_down = lambda k: (pos >= 1) & (pos + k <= n - 1)
        sends_up = lambda k: (pos <= n - 2) & (pos >= k)
        gets_down = lambda k: pos + 1 + k <= n - 1
        gets_up = lambda k: pos >= 1 + k

        def run(between=lambda k: None):
            pl.when(sends_down(0))(lambda: down(0).start())
            for k in range(n - 1):
                pl.when(gets_down(k))(lambda: down(k).wait_recv())
                if k + 1 < n - 1:
                    pl.when(sends_down(k + 1))(lambda: down(k + 1).start())
                if k > 0:
                    pl.when(gets_up(k - 1))(lambda: up(k - 1).wait_recv())
                pl.when(sends_up(k))(lambda: up(k).start())
                between(k)
            pl.when(gets_up(n - 2))(lambda: up(n - 2).wait_recv())

        def drain():
            for k in range(n - 1):
                pl.when(sends_down(k))(lambda: down(k).wait_send())
                pl.when(sends_up(k))(lambda: up(k).wait_send())

        return run, drain

    run_y, drain_y = along(
        y, Y, lambda i: rt.at[core, z, i], y_up, y_down, r2_send, r2_recv
    )
    run_z, drain_z = along(
        z, Z, lambda i: rt.at[core, i], z_up, z_down, r3_send, r3_recv
    )

    r4 = pltpu.make_async_remote_copy(
        src_ref=rt.at[core], dst_ref=rt.at[core], send_sem=r4_send, recv_sem=r4_recv,
        device_id=partner, device_id_type=MESH,
    )
    share_t = share[0]
    share_o = 1.0 - share_t

    def local(j):
        load(j, 0).wait()
        load(j, 1).wait()

        def mix(i, top):
            rows = pl.ds(pl.multiple_of(i * STEP, STEP), STEP)
            latest = share_t * tbuf[j, rows, :] + share_o * obuf[j, rows, :]
            tbuf[j, rows, :] = latest
            return jnp.maximum(top, jnp.max(jnp.abs(latest).reshape(STEP // 8, 8, WIDTH), axis=0))

        top = lax.fori_loop(0, ROWS // STEP, mix, jnp.zeros((8, WIDTH), jnp.float32), unroll=True)
        mx[j, x] = jnp.max(top, axis=0, keepdims=True)

    def finish(j):
        for k in range(3):
            max_copy(j, k).wait_recv()
        scale = jnp.maximum(
            jnp.maximum(mx[j, 0], mx[j, 1]), jnp.maximum(mx[j, 2], mx[j, 3])
        )
        sc[j // PER, :, (j % PER) * WIDTH : (j % PER + 1) * WIDTH] = scale

        def divide(i, carry):
            rows = pl.ds(pl.multiple_of(i * STEP, STEP), STEP)
            own_rows = pl.ds(pl.multiple_of(x * ROWS + i * STEP, STEP), STEP)
            out[j, own_rows, :] = (tbuf[j, rows, :] / scale).astype(jnp.bfloat16)
            return carry

        lax.fori_loop(0, ROWS // STEP, divide, 0, unroll=True)

    start_loads(0)
    for c in small:
        c.start()
    for j in range(1, CHUNKS):
        start_loads(j)
    for j in range(CHUNKS):
        local(j)
        if j == 0:
            pl.semaphore_wait(barrier, greeted)
        for k in (2, 0, 1):
            max_copy(j, k).start()
        if j == 0:
            for c in small:
                c.wait()
            piece = rwv[...] * rgv[...]
            for r in range(4):
                rt[core, z, y, x, pl.ds(r, 1), :] = piece[:, r * 128 : (r + 1) * 128]
            for k in (2, 0, 1):
                r1(k).start()
    sent = [0, 0]
    for j in range(CHUNKS):
        finish(j)
        for d in range(2):
            while sent[d] < len(OWN[d]) and sum(OWN[d][sent[d]]) <= j + 1:
                own_copy(d, sent[d]).start()
                sent[d] += 1

    for k in range(3):
        r1(k).wait_recv()
    def forward(d):
        for i in ONWARD[d][1]:
            own_copy(d, i).wait_recv()
        forward_copy(d).start()

    run_y()
    run_z(lambda k: forward(0) if k == 3 else None)
    forward(1)
    pl.when(core == 1)(lambda: r4.start())
    r4.wait_recv()
    pl.when(core == 0)(lambda: r4.start())

    def spread(zz, carry):
        rows = pl.ds(pl.multiple_of(zz * 2 * Y, 2 * Y), 2 * Y)
        for xx in range(X):
            for r in range(4):
                stage[rows, (xx * 4 + r) * 128 : (xx * 4 + r + 1) * 128] = jnp.concatenate(
                    [rt[e % 2, zz, e // 2, xx, pl.ds(r, 1), :] for e in range(2 * Y)], axis=0
                )
        return carry

    lax.fori_loop(0, Z, spread, 0)

    def narrow(i, carry):
        rows = pl.ds(pl.multiple_of(i * 16, 16), 16)
        rout[rows, :] = stage[rows, :].astype(jnp.bfloat16)
        return carry

    lax.fori_loop(0, 4, narrow, 0)

    for d in range(2):
        for i in range(len(OWN[d])):
            if i not in ONWARD[d][1]:
                own_copy(d, i).wait_recv()
            own_copy(d, i).wait_send()
    for j in range(CHUNKS):
        for k in range(3):
            max_copy(j, k).wait_send()
    for k in range(3):
        r1(k).wait_send()
    drain_y()
    drain_z()
    r4.wait_send()
    for d in range(2):
        forward_copy(d).wait_recv()
        forward_copy(d).wait_send()


def write_kernel(out, sc, rout, ready_gate, ready_up, scale_gate, scale_up, router, sem, sc_sem, r_sem):
    copies = []
    for j in range(CHUNKS):
        cols = pl.ds((j % PER) * WIDTH, WIDTH)
        copies.append(
            pltpu.make_async_copy(
                out.at[j], (ready_gate, ready_up)[j // PER].at[0, :, cols], sem.at[j]
            )
        )
    for m, scale in enumerate((scale_gate, scale_up)):
        copies.append(pltpu.make_async_copy(sc.at[m], scale, sc_sem.at[m]))
    copies.append(pltpu.make_async_copy(rout, router, r_sem))
    for c in copies:
        c.start()
    for c in copies:
        c.wait()


def per_device(train_gate, other_gate, train_up, other_up, mix_share, router_weight, router_gain):
    f32, bf16 = jnp.float32, jnp.bfloat16
    hbm = pl.BlockSpec(memory_space=pltpu.HBM)
    vmem = pl.BlockSpec(memory_space=pltpu.VMEM)
    dma = pltpu.SemaphoreType.DMA
    out, sc, rout = pl.pallas_call(
        main_kernel,
        out_shape=(
            pltpu.VMEM((CHUNKS, X * ROWS, WIDTH), bf16),
            pltpu.VMEM((2, 1, COLS), f32),
            pltpu.VMEM((2 * Y * Z, X * ROWS), bf16),
        ),
        in_specs=[pl.BlockSpec(memory_space=pltpu.SMEM)] + [hbm] * 6,
        out_specs=(vmem, vmem, vmem),
        scratch_shapes=[
            pltpu.VMEM((CHUNKS, ROWS, WIDTH), f32),
            pltpu.VMEM((CHUNKS, ROWS, WIDTH), f32),
            pltpu.VMEM((CHUNKS, X, 1, WIDTH), f32),
            pltpu.VMEM((1, ROWS), f32),
            pltpu.VMEM((1, ROWS), f32),
            pltpu.VMEM((2, Z, Y, X, 4, 128), f32),
            pltpu.VMEM((2 * Y * Z, X * ROWS), f32),
            dma((CHUNKS, 2)), dma((2,)),
            dma((CHUNKS, 3)), dma((CHUNKS, 3)),
            dma((2, 3)), dma((2, 3)), dma((2,)), dma((2,)),
            dma((3,)), dma((3,)), dma((Y - 1, 2)), dma((Y - 1, 2)),
            dma((Z - 1, 2)), dma((Z - 1, 2)),
            dma, dma,
        ],
        compiler_params=pltpu.CompilerParams(
            collective_id=0, has_side_effects=True, vmem_limit_bytes=40 * 1024 * 1024
        ),
        name="gather",
    )(
        mix_share,
        *(
            pltpu.with_memory_space_constraint(a, pltpu.HBM)
            for a in (
                train_gate, other_gate, train_up, other_up,
                router_weight.reshape(1, ROWS), router_gain.reshape(1, ROWS),
            )
        )
    )
    ready_gate, ready_up, scale_gate, scale_up, router = pl.pallas_call(
        write_kernel,
        out_shape=(
            jax.ShapeDtypeStruct((1, X * ROWS, COLS), bf16),
            jax.ShapeDtypeStruct((1, X * ROWS, COLS), bf16),
            jax.ShapeDtypeStruct((1, COLS), f32),
            jax.ShapeDtypeStruct((1, COLS), f32),
            jax.ShapeDtypeStruct((2 * Y * Z, X * ROWS), bf16),
        ),
        in_specs=[vmem] * 3,
        out_specs=(hbm,) * 5,
        scratch_shapes=[dma((CHUNKS,)), dma((2,)), dma],
        compiler_params=pltpu.CompilerParams(vmem_limit_bytes=1024 * 1024),
        name="write",
    )(*(pltpu.with_memory_space_constraint(a, pltpu.VMEM) for a in (out, sc, rout)))
    return ready_gate, ready_up, scale_gate, scale_up, router.T


def solution(mesh):
    placed = (
        P("ep", "fsdp", None),
        P("ep", "fsdp", None),
        P("ep", "fsdp", None),
        P("ep", "fsdp", None),
        P("ep"),
        P("fsdp", "ep"),
        P("fsdp"),
    )
    return jax.shard_map(
        per_device,
        mesh=mesh,
        in_specs=placed,
        out_specs=(P("ep", None, None), P("ep", None, None), P("ep", None), P("ep", None), P()),
        check_vma=False,
    )
```

```python
import functools

import jax
import jax.numpy as jnp
from jax import lax
from jax.experimental import pallas as pl
from jax.experimental.pallas import tpu as pltpu
from jax.sharding import PartitionSpec as P

MESH = pl.DeviceIdType.MESH
X, Y, Z = 4, 4, 8
ROWS, COLS = 512, 1024
WIDTH = 256
PER = COLS // WIDTH
CHUNKS = 2 * PER
OWN = (((0, 1), (1, 3), (4, 4)), ((0, 1), (4, 4), (1, 3)))
ONWARD = (((0, 4), (0, 1)), ((4, 4), (1,)))
STEP = 64
EARLY = 128


def main_kernel(
    share, tg, og, tu, ou, rw, rg,
    out, sc, rout,
    tbuf, obuf, early, mx, rwv, rgv, rt, stage,
    ld_sem, small_sem, early_send, early_recv, mx_send, mx_recv, own_send, own_recv, fwd_send, fwd_recv,
    r1_send, r1_recv, r2_send, r2_recv, r3_send, r3_recv, r4_send, r4_recv,
):
    x = lax.axis_index("fsdp")
    ep = lax.axis_index("ep")
    core = lax.rem(ep, 2)
    y = lax.rem(ep // 2, Y)
    z = ep // (2 * Y)

    right, left, opp = (lax.rem(x + k, X) for k in (1, X - 1, 2))
    x_peers = tuple({"fsdp": p} for p in (right, left, opp))
    at = lambda zz, yy, cc: {"ep": (zz * Y + yy) * 2 + cc}
    y_up, y_down = at(z, lax.rem(y + 1, Y), core), at(z, lax.rem(y + Y - 1, Y), core)
    z_up, z_down = at(lax.rem(z + 1, Z), y, core), at(lax.rem(z + Z - 1, Z), y, core)
    partner = at(z, y, 1 - core)

    barrier = pltpu.get_barrier_semaphore()

    def greet(peer):
        pl.semaphore_signal(barrier, inc=1, device_id=peer, device_id_type=MESH)

    for peer in x_peers:
        greet(peer)
    pl.when(z < Z - 1)(lambda: greet(z_up))
    pl.when(y < Y - 1)(lambda: greet(y_up))
    pl.when(core == 0)(lambda: greet(partner))
    greeted = 3 + jnp.minimum(z, 1) + jnp.minimum(y, 1) + core

    def load(j, which):
        src = ((tg, og), (tu, ou))[j // PER][which]
        cols = pl.ds((j % PER) * WIDTH, WIDTH)
        return pltpu.make_async_copy(
            src.at[0, :, cols], (tbuf, obuf)[which].at[j], ld_sem.at[j, which]
        )

    small = (
        pltpu.make_async_copy(rw, rwv, small_sem.at[0]),
        pltpu.make_async_copy(rg, rgv, small_sem.at[1]),
    )
    def start_loads(j):
        load(j, 0).start()
        load(j, 1).start()

    def max_copy(j, k):
        return pltpu.make_async_remote_copy(
            src_ref=mx.at[j, x], dst_ref=mx.at[j, x],
            send_sem=mx_send.at[j, k], recv_sem=mx_recv.at[j, k],
            device_id=x_peers[k], device_id_type=MESH,
        )

    def block(chunks, device, skip=0):
        first, number = chunks
        rows = pl.ds(pl.multiple_of(device * ROWS + skip, STEP), ROWS - skip)
        return out.at[pl.ds(first, number), rows]

    def own_copy(d, i):
        piece = block(OWN[d][i], x, EARLY if i == 0 else 0)
        return pltpu.make_async_remote_copy(
            src_ref=piece, dst_ref=piece,
            send_sem=own_send.at[d, i], recv_sem=own_recv.at[d, i],
            device_id=x_peers[d], device_id_type=MESH,
        )

    def forward_copy(d):
        piece = block(ONWARD[d][0], (left, right)[d])
        return pltpu.make_async_remote_copy(
            src_ref=piece, dst_ref=piece,
            send_sem=fwd_send.at[d], recv_sem=fwd_recv.at[d],
            device_id=x_peers[d], device_id_type=MESH,
        )

    def early_copy(d):
        return pltpu.make_async_remote_copy(
            src_ref=tbuf.at[0, pl.ds(0, EARLY)], dst_ref=early.at[d],
            send_sem=early_send.at[d], recv_sem=early_recv.at[d],
            device_id=x_peers[d], device_id_type=MESH,
        )

    def r1(k):
        ref = rt.at[core, z, y, x]
        return pltpu.make_async_remote_copy(
            src_ref=ref, dst_ref=ref, send_sem=r1_send.at[k], recv_sem=r1_recv.at[k],
            device_id=x_peers[k], device_id_type=MESH,
        )

    def line_copy(ref, peer, send_sem, recv_sem):
        return pltpu.make_async_remote_copy(
            src_ref=ref, dst_ref=ref, send_sem=send_sem, recv_sem=recv_sem,
            device_id=peer, device_id_type=MESH,
        )

    def along(pos, n, block, up_peer, down_peer, send, recv):
        down = lambda k: line_copy(
            block(lax.rem(pos + k, n)), down_peer, send.at[k, 0], recv.at[k, 0]
        )
        up = lambda k: line_copy(
            block(lax.rem(pos + n - k, n)), up_peer, send.at[k, 1], recv.at[k, 1]
        )
        sends_down = lambda k: (pos >= 1) & (pos + k <= n - 1)
        sends_up = lambda k: (pos <= n - 2) & (pos >= k)
        gets_down = lambda k: pos + 1 + k <= n - 1
        gets_up = lambda k: pos >= 1 + k

        def run(between=lambda k: None):
            pl.when(sends_down(0))(lambda: down(0).start())
            for k in range(n - 1):
                pl.when(gets_down(k))(lambda: down(k).wait_recv())
                if k + 1 < n - 1:
                    pl.when(sends_down(k + 1))(lambda: down(k + 1).start())
                if k > 0:
                    pl.when(gets_up(k - 1))(lambda: up(k - 1).wait_recv())
                pl.when(sends_up(k))(lambda: up(k).start())
                between(k)
            pl.when(gets_up(n - 2))(lambda: up(n - 2).wait_recv())

        def drain():
            for k in range(n - 1):
                pl.when(sends_down(k))(lambda: down(k).wait_send())
                pl.when(sends_up(k))(lambda: up(k).wait_send())

        return run, drain

    run_y, drain_y = along(
        y, Y, lambda i: rt.at[core, z, i], y_up, y_down, r2_send, r2_recv
    )
    run_z, drain_z = along(
        z, Z, lambda i: rt.at[core, i], z_up, z_down, r3_send, r3_recv
    )

    r4 = pltpu.make_async_remote_copy(
        src_ref=rt.at[core], dst_ref=rt.at[core], send_sem=r4_send, recv_sem=r4_recv,
        device_id=partner, device_id_type=MESH,
    )
    share_t = share[0]
    share_o = 1.0 - share_t

    def local(j):
        load(j, 0).wait()
        load(j, 1).wait()

        def mix(i, top):
            rows = pl.ds(pl.multiple_of(i * STEP, STEP), STEP)
            latest = share_t * tbuf[j, rows, :] + share_o * obuf[j, rows, :]
            tbuf[j, rows, :] = latest
            return jnp.maximum(top, jnp.max(jnp.abs(latest).reshape(STEP // 8, 8, WIDTH), axis=0))

        top = lax.fori_loop(0, ROWS // STEP, mix, jnp.zeros((8, WIDTH), jnp.float32), unroll=True)
        mx[j, x] = jnp.max(top, axis=0, keepdims=True)

    def divide(j, device, scale, source, number):
        def step(i, carry):
            rows = pl.ds(pl.multiple_of(i * STEP, STEP), STEP)
            put = pl.ds(pl.multiple_of(device * ROWS + i * STEP, STEP), STEP)
            out[j, put, :] = (source[rows, :] / scale).astype(jnp.bfloat16)
            return carry

        lax.fori_loop(0, number // STEP, step, 0, unroll=True)

    def finish(j):
        for k in range(3):
            max_copy(j, k).wait_recv()
        scale = jnp.maximum(
            jnp.maximum(mx[j, 0], mx[j, 1]), jnp.maximum(mx[j, 2], mx[j, 3])
        )
        sc[j // PER, :, (j % PER) * WIDTH : (j % PER + 1) * WIDTH] = scale

        divide(j, x, scale, tbuf.at[j], ROWS)

    for c in small:
        c.start()
    start_loads(0)
    for j in range(1, CHUNKS):
        start_loads(j)
    for j in range(CHUNKS):
        local(j)
        if j == 0:
            pl.semaphore_wait(barrier, greeted)
        for k in (2, 0, 1):
            max_copy(j, k).start()
        if j == 0:
            for d in range(2):
                early_copy(d).start()

    for c in small:
        c.wait()
    piece = rwv[...] * rgv[...]
    for r in range(4):
        rt[core, z, y, x, pl.ds(r, 1), :] = piece[:, r * 128 : (r + 1) * 128]
    for k in (2, 0, 1):
        r1(k).start()

    sent = [0, 0]
    for j in range(CHUNKS):
        finish(j)
        for d in range(2):
            while sent[d] < len(OWN[d]) and sum(OWN[d][sent[d]]) <= j + 1:
                own_copy(d, sent[d]).start()
                sent[d] += 1

    for d, source in enumerate((left, right)):
        early_copy(d).wait_recv()
        divide(0, source, sc[0, :, :WIDTH], early.at[d], EARLY)

    for k in range(3):
        r1(k).wait_recv()
    def forward(d):
        for i in ONWARD[d][1]:
            own_copy(d, i).wait_recv()
        forward_copy(d).start()

    run_y()
    run_z(lambda k: forward(0) if k == 3 else None)
    forward(1)
    pl.when(core == 1)(lambda: r4.start())
    r4.wait_recv()
    pl.when(core == 0)(lambda: r4.start())

    def spread(zz, carry):
        rows = pl.ds(pl.multiple_of(zz * 2 * Y, 2 * Y), 2 * Y)
        for xx in range(X):
            for r in range(4):
                stage[rows, (xx * 4 + r) * 128 : (xx * 4 + r + 1) * 128] = jnp.concatenate(
                    [rt[e % 2, zz, e // 2, xx, pl.ds(r, 1), :] for e in range(2 * Y)], axis=0
                )
        return carry

    lax.fori_loop(0, Z, spread, 0)

    def narrow(i, carry):
        rows = pl.ds(pl.multiple_of(i * 16, 16), 16)
        rout[rows, :] = stage[rows, :].astype(jnp.bfloat16)
        return carry

    lax.fori_loop(0, 4, narrow, 0)

    for d in range(2):
        for i in range(len(OWN[d])):
            if i not in ONWARD[d][1]:
                own_copy(d, i).wait_recv()
            own_copy(d, i).wait_send()
    for j in range(CHUNKS):
        for k in range(3):
            max_copy(j, k).wait_send()
    for k in range(3):
        r1(k).wait_send()
    for d in range(2):
        early_copy(d).wait_send()
    drain_y()
    drain_z()
    r4.wait_send()
    for d in range(2):
        forward_copy(d).wait_recv()
        forward_copy(d).wait_send()


def write_kernel(out, sc, rout, ready_gate, ready_up, scale_gate, scale_up, router, sem, sc_sem, r_sem):
    copies = []
    for j in range(CHUNKS):
        cols = pl.ds((j % PER) * WIDTH, WIDTH)
        copies.append(
            pltpu.make_async_copy(
                out.at[j], (ready_gate, ready_up)[j // PER].at[0, :, cols], sem.at[j]
            )
        )
    for m, scale in enumerate((scale_gate, scale_up)):
        copies.append(pltpu.make_async_copy(sc.at[m], scale, sc_sem.at[m]))
    copies.append(pltpu.make_async_copy(rout, router, r_sem))
    for c in copies:
        c.start()
    for c in copies:
        c.wait()


def per_device(train_gate, other_gate, train_up, other_up, mix_share, router_weight, router_gain):
    f32, bf16 = jnp.float32, jnp.bfloat16
    hbm = pl.BlockSpec(memory_space=pltpu.HBM)
    vmem = pl.BlockSpec(memory_space=pltpu.VMEM)
    dma = pltpu.SemaphoreType.DMA
    out, sc, rout = pl.pallas_call(
        main_kernel,
        out_shape=(
            pltpu.VMEM((CHUNKS, X * ROWS, WIDTH), bf16),
            pltpu.VMEM((2, 1, COLS), f32),
            pltpu.VMEM((2 * Y * Z, X * ROWS), bf16),
        ),
        in_specs=[pl.BlockSpec(memory_space=pltpu.SMEM)] + [hbm] * 6,
        out_specs=(vmem, vmem, vmem),
        scratch_shapes=[
            pltpu.VMEM((CHUNKS, ROWS, WIDTH), f32),
            pltpu.VMEM((CHUNKS, ROWS, WIDTH), f32),
            pltpu.VMEM((2, EARLY, WIDTH), f32),
            pltpu.VMEM((CHUNKS, X, 1, WIDTH), f32),
            pltpu.VMEM((1, ROWS), f32),
            pltpu.VMEM((1, ROWS), f32),
            pltpu.VMEM((2, Z, Y, X, 4, 128), f32),
            pltpu.VMEM((2 * Y * Z, X * ROWS), f32),
            dma((CHUNKS, 2)), dma((2,)), dma((2,)), dma((2,)),
            dma((CHUNKS, 3)), dma((CHUNKS, 3)),
            dma((2, 3)), dma((2, 3)), dma((2,)), dma((2,)),
            dma((3,)), dma((3,)), dma((Y - 1, 2)), dma((Y - 1, 2)),
            dma((Z - 1, 2)), dma((Z - 1, 2)),
            dma, dma,
        ],
        compiler_params=pltpu.CompilerParams(
            collective_id=0, has_side_effects=True, vmem_limit_bytes=40 * 1024 * 1024
        ),
        name="gather",
    )(
        mix_share,
        *(
            pltpu.with_memory_space_constraint(a, pltpu.HBM)
            for a in (
                train_gate, other_gate, train_up, other_up,
                router_weight.reshape(1, ROWS), router_gain.reshape(1, ROWS),
            )
        )
    )
    ready_gate, ready_up, scale_gate, scale_up, router = pl.pallas_call(
        write_kernel,
        out_shape=(
            jax.ShapeDtypeStruct((1, X * ROWS, COLS), bf16),
            jax.ShapeDtypeStruct((1, X * ROWS, COLS), bf16),
            jax.ShapeDtypeStruct((1, COLS), f32),
            jax.ShapeDtypeStruct((1, COLS), f32),
            jax.ShapeDtypeStruct((2 * Y * Z, X * ROWS), bf16),
        ),
        in_specs=[vmem] * 3,
        out_specs=(hbm,) * 5,
        scratch_shapes=[dma((CHUNKS,)), dma((2,)), dma],
        compiler_params=pltpu.CompilerParams(vmem_limit_bytes=1024 * 1024),
        name="write",
    )(*(pltpu.with_memory_space_constraint(a, pltpu.VMEM) for a in (out, sc, rout)))
    return ready_gate, ready_up, scale_gate, scale_up, router.T


def solution(mesh):
    placed = (
        P("ep", "fsdp", None),
        P("ep", "fsdp", None),
        P("ep", "fsdp", None),
        P("ep", "fsdp", None),
        P("ep"),
        P("fsdp", "ep"),
        P("fsdp"),
    )
    return jax.shard_map(
        per_device,
        mesh=mesh,
        in_specs=placed,
        out_specs=(P("ep", None, None), P("ep", None, None), P("ep", None), P("ep", None), P()),
        check_vma=False,
    )
```

```python
import functools

import jax
import jax.numpy as jnp
from jax import lax
from jax.experimental import pallas as pl
from jax.experimental.pallas import tpu as pltpu
from jax.sharding import PartitionSpec as P

MESH = pl.DeviceIdType.MESH
X, Y, Z = 4, 4, 8
ROWS, COLS = 512, 1024
WIDTH = 256
PER = COLS // WIDTH
CHUNKS = 2 * PER
GROUPS = ((0, 1), (1, 3), (4, 4))
OWN = (((0, 1), (1, 3), (4, 4)), ((0, 1), (4, 4), (1, 3)))
ONWARD = (((0, 4), (0, 1)), ((4, 4), (1,)))
STEP = 64
EARLY = 128


def main_kernel(
    share, tg, og, tu, ou, rw, rg,
    out, sc, rout,
    buf, early, mx, rgw, rt, stage,
    ld_sem, small_sem, early_send, early_recv, mx_send, mx_recv,
    own_send, own_recv, fwd_send, fwd_recv,
    r1_send, r1_recv, r2_send, r2_recv, r3_send, r3_recv, r4_send, r4_recv,
):
    x = lax.axis_index("fsdp")
    ep = lax.axis_index("ep")
    core = lax.rem(ep, 2)
    y = lax.rem(ep // 2, Y)
    z = ep // (2 * Y)

    right, left, opp = (lax.rem(x + k, X) for k in (1, X - 1, 2))
    x_peers = tuple({"fsdp": p} for p in (right, left, opp))
    at = lambda zz, yy, cc: {"ep": (zz * Y + yy) * 2 + cc}
    y_up, y_down = at(z, lax.rem(y + 1, Y), core), at(z, lax.rem(y + Y - 1, Y), core)
    z_up, z_down = at(lax.rem(z + 1, Z), y, core), at(lax.rem(z + Z - 1, Z), y, core)
    partner = at(z, y, 1 - core)

    barrier = pltpu.get_barrier_semaphore()

    def greet(peer):
        pl.semaphore_signal(barrier, inc=1, device_id=peer, device_id_type=MESH)

    for peer in x_peers:
        greet(peer)
    pl.when(z < Z - 1)(lambda: greet(z_up))
    pl.when(y < Y - 1)(lambda: greet(y_up))
    pl.when(core == 0)(lambda: greet(partner))
    greeted = 3 + jnp.minimum(z, 1) + jnp.minimum(y, 1) + core

    small = (
        pltpu.make_async_copy(rw, rgw.at[0], small_sem),
        pltpu.make_async_copy(rg, rgw.at[1], small_sem),
    )

    def start_loads(g):
        first, number = GROUPS[g]
        for j in range(first, first + number):
            cols = pl.ds((j % PER) * WIDTH, WIDTH)
            for which, src in enumerate(((tg, og), (tu, ou))[j // PER]):
                pltpu.make_async_copy(src.at[0, :, cols], buf.at[which, j], ld_sem.at[g]).start()

    def wait_loads(g):
        all_of_it = buf.at[:, pl.ds(*GROUPS[g])]
        pltpu.make_async_copy(all_of_it, all_of_it, ld_sem.at[g]).wait()

    def as_many(ref, sem):
        return pltpu.make_async_remote_copy(
            src_ref=ref, dst_ref=ref, send_sem=sem, recv_sem=sem,
            device_id=x_peers[0], device_id_type=MESH,
        )

    def out_rows(number, rows):
        return out.at[pl.ds(0, number), pl.ds(0, rows)]

    def max_copy(g, k):
        mine = mx.at[pl.ds(*GROUPS[g]), x]
        return pltpu.make_async_remote_copy(
            src_ref=mine, dst_ref=mine, send_sem=mx_send, recv_sem=mx_recv.at[g],
            device_id=x_peers[k], device_id_type=MESH,
        )

    def block(chunks, device, skip=0):
        first, number = chunks
        rows = pl.ds(pl.multiple_of(device * ROWS + skip, STEP), ROWS - skip)
        return out.at[pl.ds(first, number), rows]

    def own_copy(d, i):
        piece = block(OWN[d][i], x, EARLY if i == 0 else 0)
        return pltpu.make_async_remote_copy(
            src_ref=piece, dst_ref=piece,
            send_sem=own_send, recv_sem=own_recv.at[d, 0 if i in ONWARD[d][1] else 1],
            device_id=x_peers[d], device_id_type=MESH,
        )

    def forward_copy(d):
        piece = block(ONWARD[d][0], (left, right)[d])
        return pltpu.make_async_remote_copy(
            src_ref=piece, dst_ref=piece,
            send_sem=fwd_send, recv_sem=fwd_recv,
            device_id=x_peers[d], device_id_type=MESH,
        )

    def early_copy(d):
        return pltpu.make_async_remote_copy(
            src_ref=buf.at[0, 0, pl.ds(0, EARLY)], dst_ref=early.at[d],
            send_sem=early_send, recv_sem=early_recv,
            device_id=x_peers[d], device_id_type=MESH,
        )

    def r1(k):
        ref = rt.at[core, z, y, x]
        return pltpu.make_async_remote_copy(
            src_ref=ref, dst_ref=ref, send_sem=r1_send, recv_sem=r1_recv,
            device_id=x_peers[k], device_id_type=MESH,
        )

    def line_copy(ref, peer, send_sem, recv_sem):
        return pltpu.make_async_remote_copy(
            src_ref=ref, dst_ref=ref, send_sem=send_sem, recv_sem=recv_sem,
            device_id=peer, device_id_type=MESH,
        )

    def along(pos, n, block, up_peer, down_peer, send, recv):
        down = lambda k: line_copy(
            block(lax.rem(pos + k, n)), down_peer, send.at[0], recv.at[k, 0]
        )
        up = lambda k: line_copy(
            block(lax.rem(pos + n - k, n)), up_peer, send.at[1], recv.at[k, 1]
        )
        sends_down = lambda k: (pos >= 1) & (pos + k <= n - 1)
        sends_up = lambda k: (pos <= n - 2) & (pos >= k)
        gets_down = lambda k: pos + 1 + k <= n - 1
        gets_up = lambda k: pos >= 1 + k

        def next_down(k):
            if k > 0:
                down(k - 1).wait_send()
            down(k).start()

        def next_up(k):
            if k > 0:
                up(k - 1).wait_send()
            up(k).start()

        def run(between=lambda k: None):
            pl.when(sends_down(0))(lambda: next_down(0))
            for k in range(n - 1):
                pl.when(gets_down(k))(lambda: down(k).wait_recv())
                if k + 1 < n - 1:
                    pl.when(sends_down(k + 1))(lambda: next_down(k + 1))
                if k > 0:
                    pl.when(gets_up(k - 1))(lambda: up(k - 1).wait_recv())
                pl.when(sends_up(k))(lambda: next_up(k))
                between(k)
            pl.when(gets_up(n - 2))(lambda: up(n - 2).wait_recv())

        def drain():
            pl.when(sends_down(0))(lambda: down(0).wait_send())
            pl.when(sends_up(0))(lambda: up(0).wait_send())

        return run, drain

    run_y, drain_y = along(
        y, Y, lambda i: rt.at[core, z, i], y_up, y_down, r2_send, r2_recv
    )
    run_z, drain_z = along(
        z, Z, lambda i: rt.at[core, i], z_up, z_down, r3_send, r3_recv
    )

    r4 = pltpu.make_async_remote_copy(
        src_ref=rt.at[core], dst_ref=rt.at[core], send_sem=r4_send, recv_sem=r4_recv,
        device_id=partner, device_id_type=MESH,
    )
    share_t = share[0]
    share_o = 1.0 - share_t

    def local(j):
        def mix(i, top):
            rows = pl.ds(pl.multiple_of(i * STEP, STEP), STEP)
            latest = share_t * buf[0, j, rows, :] + share_o * buf[1, j, rows, :]
            buf[0, j, rows, :] = latest
            return jnp.maximum(top, jnp.max(jnp.abs(latest).reshape(STEP // 8, 8, WIDTH), axis=0))

        top = lax.fori_loop(0, ROWS // STEP, mix, jnp.zeros((8, WIDTH), jnp.float32), unroll=True)
        mx[j, x] = jnp.max(top, axis=0, keepdims=True)

    def divide(j, device, scale, source, number):
        def step(i, carry):
            rows = pl.ds(pl.multiple_of(i * STEP, STEP), STEP)
            put = pl.ds(pl.multiple_of(device * ROWS + i * STEP, STEP), STEP)
            out[j, put, :] = (source[rows, :] / scale).astype(jnp.bfloat16)
            return carry

        lax.fori_loop(0, number // STEP, step, 0, unroll=True)

    def finish(j):
        scale = jnp.maximum(
            jnp.maximum(mx[j, 0], mx[j, 1]), jnp.maximum(mx[j, 2], mx[j, 3])
        )
        sc[j // PER, :, (j % PER) * WIDTH : (j % PER + 1) * WIDTH] = scale

        divide(j, x, scale, buf.at[0, j], ROWS)

    for c in small:
        c.start()
    for g in range(len(GROUPS)):
        start_loads(g)
    for g, (first, number) in enumerate(GROUPS):
        wait_loads(g)
        for j in range(first, first + number):
            local(j)
        if g == 0:
            pl.semaphore_wait(barrier, greeted)
        for k in (2, 0, 1):
            max_copy(g, k).start()
        if g == 0:
            for d in range(2):
                early_copy(d).start()

    pltpu.make_async_copy(rgw, rgw, small_sem).wait()
    piece = rgw[0] * rgw[1]
    for r in range(4):
        rt[core, z, y, x, pl.ds(r, 1), :] = piece[:, r * 128 : (r + 1) * 128]
    for k in (2, 0, 1):
        r1(k).start()

    sent = [0, 0]
    for j in range(CHUNKS):
        for g, (first, number) in enumerate(GROUPS):
            if j == first:
                as_many(mx.at[pl.ds(first, number), pl.ds(0, X - 1)], mx_recv.at[g]).wait_recv()
        finish(j)
        for d in range(2):
            while sent[d] < len(OWN[d]) and sum(OWN[d][sent[d]]) <= j + 1:
                own_copy(d, sent[d]).start()
                sent[d] += 1

    as_many(early, early_recv).wait_recv()
    for d, source in enumerate((left, right)):
        divide(0, source, sc[0, :, :WIDTH], early.at[d], EARLY)

    r1_all = as_many(rt.at[core, z, y, pl.ds(0, X - 1)], r1_recv)
    r1_all.wait_recv()
    own_rows = CHUNKS * ROWS - EARLY
    onward_rows = [
        sum(OWN[d][i][1] * ROWS - (EARLY if i == 0 else 0) for i in ONWARD[d][1]) for d in range(2)
    ]

    def forward(d):
        as_many(out_rows(1, onward_rows[d]), own_recv.at[d, 0]).wait_recv()
        forward_copy(d).start()

    run_y()
    run_z(lambda k: forward(0) if k == 3 else None)
    forward(1)
    pl.when(core == 1)(lambda: r4.start())
    r4.wait_recv()
    pl.when(core == 0)(lambda: r4.start())

    def spread(zz, carry):
        rows = pl.ds(pl.multiple_of(zz * 2 * Y, 2 * Y), 2 * Y)
        for xx in range(X):
            for r in range(4):
                stage[rows, (xx * 4 + r) * 128 : (xx * 4 + r + 1) * 128] = jnp.concatenate(
                    [rt[e % 2, zz, e // 2, xx, pl.ds(r, 1), :] for e in range(2 * Y)], axis=0
                )
        return carry

    lax.fori_loop(0, Z, spread, 0)

    def narrow(i, carry):
        rows = pl.ds(pl.multiple_of(i * 16, 16), 16)
        rout[rows, :] = stage[rows, :].astype(jnp.bfloat16)
        return carry

    lax.fori_loop(0, 4, narrow, 0)

    for d in range(2):
        as_many(out_rows(1, own_rows - onward_rows[d]), own_recv.at[d, 1]).wait_recv()
    as_many(out_rows(4, own_rows // 2), own_send).wait_send()
    as_many(mx.at[:, pl.ds(0, X - 1)], mx_send).wait_send()
    as_many(rt.at[core, z, y, pl.ds(0, X - 1)], r1_send).wait_send()
    as_many(early, early_send).wait_send()
    drain_y()
    drain_z()
    r4.wait_send()
    as_many(out_rows(2, X * ROWS), fwd_recv).wait_recv()
    as_many(out_rows(2, X * ROWS), fwd_send).wait_send()


def write_kernel(out, sc, rout, ready_gate, ready_up, scale_gate, scale_up, router, sem, sc_sem, r_sem):
    for j in range(CHUNKS):
        cols = pl.ds((j % PER) * WIDTH, WIDTH)
        ready = (ready_gate, ready_up)[j // PER]
        pltpu.make_async_copy(out.at[j], ready.at[0, :, cols], sem).start()
    for m, scale in enumerate((scale_gate, scale_up)):
        pltpu.make_async_copy(sc.at[m], scale, sc_sem).start()
    routed = pltpu.make_async_copy(rout, router, r_sem)
    routed.start()
    pltpu.make_async_copy(sc, sc, sc_sem).wait()
    routed.wait()
    pltpu.make_async_copy(out, out, sem).wait()


def per_device(train_gate, other_gate, train_up, other_up, mix_share, router_weight, router_gain):
    f32, bf16 = jnp.float32, jnp.bfloat16
    hbm = pl.BlockSpec(memory_space=pltpu.HBM)
    vmem = pl.BlockSpec(memory_space=pltpu.VMEM)
    dma = pltpu.SemaphoreType.DMA
    out, sc, rout = pl.pallas_call(
        main_kernel,
        out_shape=(
            pltpu.VMEM((CHUNKS, X * ROWS, WIDTH), bf16),
            pltpu.VMEM((2, 1, COLS), f32),
            pltpu.VMEM((2 * Y * Z, X * ROWS), bf16),
        ),
        in_specs=[pl.BlockSpec(memory_space=pltpu.SMEM)] + [hbm] * 6,
        out_specs=(vmem, vmem, vmem),
        scratch_shapes=[
            pltpu.VMEM((2, CHUNKS, ROWS, WIDTH), f32),
            pltpu.VMEM((2, EARLY, WIDTH), f32),
            pltpu.VMEM((CHUNKS, X, 1, WIDTH), f32),
            pltpu.VMEM((2, 1, ROWS), f32),
            pltpu.VMEM((2, Z, Y, X, 4, 128), f32),
            pltpu.VMEM((2 * Y * Z, X * ROWS), f32),
            dma((len(GROUPS),)), dma, dma, dma, dma, dma((len(GROUPS),)),
            dma, dma((2, 2)), dma, dma,
            dma, dma, dma((2,)), dma((Y - 1, 2)), dma((2,)), dma((Z - 1, 2)), dma, dma,
        ],
        compiler_params=pltpu.CompilerParams(
            collective_id=0, has_side_effects=True, vmem_limit_bytes=40 * 1024 * 1024
        ),
        name="gather",
    )(
        mix_share,
        *(
            pltpu.with_memory_space_constraint(a, pltpu.HBM)
            for a in (
                train_gate, other_gate, train_up, other_up,
                router_weight.reshape(1, ROWS), router_gain.reshape(1, ROWS),
            )
        )
    )
    ready_gate, ready_up, scale_gate, scale_up, router = pl.pallas_call(
        write_kernel,
        out_shape=(
            jax.ShapeDtypeStruct((1, X * ROWS, COLS), bf16),
            jax.ShapeDtypeStruct((1, X * ROWS, COLS), bf16),
            jax.ShapeDtypeStruct((1, COLS), f32),
            jax.ShapeDtypeStruct((1, COLS), f32),
            jax.ShapeDtypeStruct((2 * Y * Z, X * ROWS), bf16),
        ),
        in_specs=[vmem] * 3,
        out_specs=(hbm,) * 5,
        scratch_shapes=[dma, dma, dma],
        compiler_params=pltpu.CompilerParams(vmem_limit_bytes=1024 * 1024),
        name="write",
    )(*(pltpu.with_memory_space_constraint(a, pltpu.VMEM) for a in (out, sc, rout)))
    return ready_gate, ready_up, scale_gate, scale_up, router.T


def solution(mesh):
    placed = (
        P("ep", "fsdp", None),
        P("ep", "fsdp", None),
        P("ep", "fsdp", None),
        P("ep", "fsdp", None),
        P("ep"),
        P("fsdp", "ep"),
        P("fsdp"),
    )
    return jax.shard_map(
        per_device,
        mesh=mesh,
        in_specs=placed,
        out_specs=(P("ep", None, None), P("ep", None, None), P("ep", None), P("ep", None), P()),
        check_vma=False,
    )
```

```python
import functools

import jax
import jax.numpy as jnp
from jax import lax
from jax.experimental import pallas as pl
from jax.experimental.pallas import tpu as pltpu
from jax.sharding import PartitionSpec as P

MESH = pl.DeviceIdType.MESH
X, Y, Z = 4, 4, 8
ROWS, COLS = 512, 1024
WIDTH = 256
PER = COLS // WIDTH
CHUNKS = 2 * PER
GROUPS = ((0, 1), (1, 3), (4, 4))
OWN = (((0, 1), (1, 3), (4, 4)), ((0, 1), (4, 4), (1, 3)))
ONWARD = (((0, 4), (0, 1)), ((4, 4), (1,)))
STEP = 16
EARLY = 112


def main_kernel(
    share, tg, og, tu, ou, rw, rg,
    out, sc, rout,
    buf, early, mx, rgw, rt, stage,
    ld_sem, small_sem, early_send, early_recv, mx_send, mx_recv,
    own_send, own_recv, fwd_send, fwd_recv,
    r1_send, r1_recv, r2_send, r2_recv, r3_send, r3_recv, r4_send, r4_recv,
):
    x = lax.axis_index("fsdp")
    ep = lax.axis_index("ep")
    core = lax.rem(ep, 2)
    y = lax.rem(ep // 2, Y)
    z = ep // (2 * Y)

    right, left, opp = (lax.rem(x + k, X) for k in (1, X - 1, 2))
    x_peers = tuple({"fsdp": p} for p in (right, left, opp))
    at = lambda zz, yy, cc: {"ep": (zz * Y + yy) * 2 + cc}
    y_up, y_down = at(z, lax.rem(y + 1, Y), core), at(z, lax.rem(y + Y - 1, Y), core)
    z_up, z_down = at(lax.rem(z + 1, Z), y, core), at(lax.rem(z + Z - 1, Z), y, core)
    partner = at(z, y, 1 - core)

    barrier = pltpu.get_barrier_semaphore()

    def greet(peer):
        pl.semaphore_signal(barrier, inc=1, device_id=peer, device_id_type=MESH)

    for peer in (x_peers[2], x_peers[0], x_peers[1]):
        greet(peer)

    small = (
        pltpu.make_async_copy(rw, rgw.at[0], small_sem),
        pltpu.make_async_copy(rg, rgw.at[1], small_sem),
    )

    def start_loads(g):
        first, number = GROUPS[g]
        for j in range(first, first + number):
            cols = pl.ds((j % PER) * WIDTH, WIDTH)
            for which, src in enumerate(((tg, og), (tu, ou))[j // PER]):
                pltpu.make_async_copy(src.at[0, :, cols], buf.at[which, j], ld_sem.at[g]).start()

    def wait_loads(g):
        all_of_it = buf.at[:, pl.ds(*GROUPS[g])]
        pltpu.make_async_copy(all_of_it, all_of_it, ld_sem.at[g]).wait()

    def as_many(ref, sem):
        return pltpu.make_async_remote_copy(
            src_ref=ref, dst_ref=ref, send_sem=sem, recv_sem=sem,
            device_id=x_peers[0], device_id_type=MESH,
        )

    def out_rows(number, rows):
        return out.at[pl.ds(0, number), pl.ds(0, rows)]

    def max_copy(g, k):
        mine = mx.at[pl.ds(*GROUPS[g]), x]
        return pltpu.make_async_remote_copy(
            src_ref=mine, dst_ref=mine, send_sem=mx_send, recv_sem=mx_recv.at[g],
            device_id=x_peers[k], device_id_type=MESH,
        )

    def block(chunks, device, skip=0):
        first, number = chunks
        rows = pl.ds(pl.multiple_of(device * ROWS + skip, STEP), ROWS - skip)
        return out.at[pl.ds(first, number), rows]

    def own_copy(d, i):
        piece = block(OWN[d][i], x, EARLY if i == 0 else 0)
        return pltpu.make_async_remote_copy(
            src_ref=piece, dst_ref=piece,
            send_sem=own_send, recv_sem=own_recv.at[d, 0 if i in ONWARD[d][1] else 1],
            device_id=x_peers[d], device_id_type=MESH,
        )

    def forward_copy(d):
        piece = block(ONWARD[d][0], (left, right)[d])
        return pltpu.make_async_remote_copy(
            src_ref=piece, dst_ref=piece,
            send_sem=fwd_send, recv_sem=fwd_recv,
            device_id=x_peers[d], device_id_type=MESH,
        )

    def early_copy(d):
        return pltpu.make_async_remote_copy(
            src_ref=buf.at[0, 0, pl.ds(0, EARLY)], dst_ref=early.at[d],
            send_sem=early_send, recv_sem=early_recv,
            device_id=x_peers[d], device_id_type=MESH,
        )

    def r1(k):
        ref = rt.at[core, z, y, x]
        return pltpu.make_async_remote_copy(
            src_ref=ref, dst_ref=ref, send_sem=r1_send, recv_sem=r1_recv,
            device_id=x_peers[k], device_id_type=MESH,
        )

    def line_copy(ref, peer, send_sem, recv_sem):
        return pltpu.make_async_remote_copy(
            src_ref=ref, dst_ref=ref, send_sem=send_sem, recv_sem=recv_sem,
            device_id=peer, device_id_type=MESH,
        )

    def along(pos, n, block, up_peer, down_peer, send, recv):
        down = lambda k: line_copy(
            block(lax.rem(pos + k, n)), down_peer, send.at[0], recv.at[k, 0]
        )
        up = lambda k: line_copy(
            block(lax.rem(pos + n - k, n)), up_peer, send.at[1], recv.at[k, 1]
        )
        sends_down = lambda k: (pos >= 1) & (pos + k <= n - 1)
        sends_up = lambda k: (pos <= n - 2) & (pos >= k)
        gets_down = lambda k: pos + 1 + k <= n - 1
        gets_up = lambda k: pos >= 1 + k

        def next_down(k):
            if k > 0:
                down(k - 1).wait_send()
            down(k).start()

        def next_up(k):
            if k > 0:
                up(k - 1).wait_send()
            up(k).start()

        def run(between=lambda k: None):
            pl.when(sends_down(0))(lambda: next_down(0))
            for k in range(n - 1):
                pl.when(gets_down(k))(lambda: down(k).wait_recv())
                if k + 1 < n - 1:
                    pl.when(sends_down(k + 1))(lambda: next_down(k + 1))
                if k > 0:
                    pl.when(gets_up(k - 1))(lambda: up(k - 1).wait_recv())
                pl.when(sends_up(k))(lambda: next_up(k))
                between(k)
            pl.when(gets_up(n - 2))(lambda: up(n - 2).wait_recv())

        def drain():
            pl.when(sends_down(0))(lambda: down(0).wait_send())
            pl.when(sends_up(0))(lambda: up(0).wait_send())

        return run, drain

    run_y, drain_y = along(
        y, Y, lambda i: rt.at[core, z, i], y_up, y_down, r2_send, r2_recv
    )
    run_z, drain_z = along(
        z, Z, lambda i: rt.at[core, i], z_up, z_down, r3_send, r3_recv
    )

    r4 = pltpu.make_async_remote_copy(
        src_ref=rt.at[core], dst_ref=rt.at[core], send_sem=r4_send, recv_sem=r4_recv,
        device_id=partner, device_id_type=MESH,
    )
    share_t = share[0]
    share_o = 1.0 - share_t

    def local(j):
        def mix(i, top):
            rows = pl.ds(pl.multiple_of(i * STEP, STEP), STEP)
            latest = share_t * buf[0, j, rows, :] + share_o * buf[1, j, rows, :]
            buf[0, j, rows, :] = latest
            return jnp.maximum(top, jnp.max(jnp.abs(latest).reshape(STEP // 8, 8, WIDTH), axis=0))

        top = lax.fori_loop(0, ROWS // STEP, mix, jnp.zeros((8, WIDTH), jnp.float32), unroll=True)
        mx[j, x] = jnp.max(top, axis=0, keepdims=True)

    def divide(j, device, scale, source, number):
        def step(i, carry):
            rows = pl.ds(pl.multiple_of(i * STEP, STEP), STEP)
            put = pl.ds(pl.multiple_of(device * ROWS + i * STEP, STEP), STEP)
            out[j, put, :] = (source[rows, :] / scale).astype(jnp.bfloat16)
            return carry

        lax.fori_loop(0, number // STEP, step, 0, unroll=True)

    def finish(j):
        scale = jnp.maximum(
            jnp.maximum(mx[j, 0], mx[j, 1]), jnp.maximum(mx[j, 2], mx[j, 3])
        )
        sc[j // PER, :, (j % PER) * WIDTH : (j % PER + 1) * WIDTH] = scale

        divide(j, x, scale, buf.at[0, j], ROWS)

    start_loads(0)
    pl.when(z < Z - 1)(lambda: greet(z_up))
    pl.when(y < Y - 1)(lambda: greet(y_up))
    pl.when(core == 0)(lambda: greet(partner))
    greeted = 3 + jnp.minimum(z, 1) + jnp.minimum(y, 1) + core
    for c in small:
        c.start()
    for g in range(1, len(GROUPS)):
        start_loads(g)
    for g, (first, number) in enumerate(GROUPS):
        wait_loads(g)
        for j in range(first, first + number):
            local(j)
        if g == 0:
            pl.semaphore_wait(barrier, greeted)
        for k in (2, 0, 1):
            max_copy(g, k).start()
        if g == 0:
            for d in range(2):
                early_copy(d).start()

    pltpu.make_async_copy(rgw, rgw, small_sem).wait()
    piece = rgw[0] * rgw[1]
    for r in range(4):
        rt[core, z, y, x, pl.ds(r, 1), :] = piece[:, r * 128 : (r + 1) * 128]
    for k in (2, 0, 1):
        r1(k).start()

    sent = [0, 0]
    for j in range(CHUNKS):
        for g, (first, number) in enumerate(GROUPS):
            if j == first:
                as_many(mx.at[pl.ds(first, number), pl.ds(0, X - 1)], mx_recv.at[g]).wait_recv()
        finish(j)
        for d in range(2):
            while sent[d] < len(OWN[d]) and sum(OWN[d][sent[d]]) <= j + 1:
                own_copy(d, sent[d]).start()
                sent[d] += 1

    as_many(early, early_recv).wait_recv()
    for d, source in enumerate((left, right)):
        divide(0, source, sc[0, :, :WIDTH], early.at[d], EARLY)

    r1_all = as_many(rt.at[core, z, y, pl.ds(0, X - 1)], r1_recv)
    r1_all.wait_recv()
    own_rows = CHUNKS * ROWS - EARLY
    onward_rows = [
        sum(OWN[d][i][1] * ROWS - (EARLY if i == 0 else 0) for i in ONWARD[d][1]) for d in range(2)
    ]

    def forward(d):
        as_many(out_rows(1, onward_rows[d]), own_recv.at[d, 0]).wait_recv()
        forward_copy(d).start()

    run_y()
    run_z(lambda k: forward(0) if k == 3 else None)
    forward(1)
    pl.when(core == 1)(lambda: r4.start())
    r4.wait_recv()
    pl.when(core == 0)(lambda: r4.start())

    def spread(zz, carry):
        rows = pl.ds(pl.multiple_of(zz * 2 * Y, 2 * Y), 2 * Y)
        for xx in range(X):
            for r in range(4):
                stage[rows, (xx * 4 + r) * 128 : (xx * 4 + r + 1) * 128] = jnp.concatenate(
                    [rt[e % 2, zz, e // 2, xx, pl.ds(r, 1), :] for e in range(2 * Y)], axis=0
                )
        return carry

    lax.fori_loop(0, Z, spread, 0)

    def narrow(i, carry):
        rows = pl.ds(pl.multiple_of(i * 16, 16), 16)
        rout[rows, :] = stage[rows, :].astype(jnp.bfloat16)
        return carry

    lax.fori_loop(0, 4, narrow, 0)

    for d in range(2):
        as_many(out_rows(1, own_rows - onward_rows[d]), own_recv.at[d, 1]).wait_recv()
    as_many(out_rows(4, own_rows // 2), own_send).wait_send()
    as_many(mx.at[:, pl.ds(0, X - 1)], mx_send).wait_send()
    as_many(rt.at[core, z, y, pl.ds(0, X - 1)], r1_send).wait_send()
    as_many(early, early_send).wait_send()
    drain_y()
    drain_z()
    r4.wait_send()
    as_many(out_rows(2, X * ROWS), fwd_recv).wait_recv()
    as_many(out_rows(2, X * ROWS), fwd_send).wait_send()


def write_kernel(out, sc, rout, ready_gate, ready_up, scale_gate, scale_up, router, sem, sc_sem, r_sem):
    for j in range(CHUNKS):
        cols = pl.ds((j % PER) * WIDTH, WIDTH)
        ready = (ready_gate, ready_up)[j // PER]
        pltpu.make_async_copy(out.at[j], ready.at[0, :, cols], sem).start()
    for m, scale in enumerate((scale_gate, scale_up)):
        pltpu.make_async_copy(sc.at[m], scale, sc_sem).start()
    routed = pltpu.make_async_copy(rout, router, r_sem)
    routed.start()
    pltpu.make_async_copy(sc, sc, sc_sem).wait()
    routed.wait()
    pltpu.make_async_copy(out, out, sem).wait()


def per_device(train_gate, other_gate, train_up, other_up, mix_share, router_weight, router_gain):
    f32, bf16 = jnp.float32, jnp.bfloat16
    hbm = pl.BlockSpec(memory_space=pltpu.HBM)
    vmem = pl.BlockSpec(memory_space=pltpu.VMEM)
    dma = pltpu.SemaphoreType.DMA
    out, sc, rout = pl.pallas_call(
        main_kernel,
        out_shape=(
            pltpu.VMEM((CHUNKS, X * ROWS, WIDTH), bf16),
            pltpu.VMEM((2, 1, COLS), f32),
            pltpu.VMEM((2 * Y * Z, X * ROWS), bf16),
        ),
        in_specs=[pl.BlockSpec(memory_space=pltpu.SMEM)] + [hbm] * 6,
        out_specs=(vmem, vmem, vmem),
        scratch_shapes=[
            pltpu.VMEM((2, CHUNKS, ROWS, WIDTH), f32),
            pltpu.VMEM((2, EARLY, WIDTH), f32),
            pltpu.VMEM((CHUNKS, X, 1, WIDTH), f32),
            pltpu.VMEM((2, 1, ROWS), f32),
            pltpu.VMEM((2, Z, Y, X, 4, 128), f32),
            pltpu.VMEM((2 * Y * Z, X * ROWS), f32),
            dma((len(GROUPS),)), dma, dma, dma, dma, dma((len(GROUPS),)),
            dma, dma((2, 2)), dma, dma,
            dma, dma, dma((2,)), dma((Y - 1, 2)), dma((2,)), dma((Z - 1, 2)), dma, dma,
        ],
        compiler_params=pltpu.CompilerParams(
            collective_id=0, has_side_effects=True, vmem_limit_bytes=40 * 1024 * 1024
        ),
        name="gather",
    )(
        mix_share,
        *(
            pltpu.with_memory_space_constraint(a, pltpu.HBM)
            for a in (
                train_gate, other_gate, train_up, other_up,
                router_weight.reshape(1, ROWS), router_gain.reshape(1, ROWS),
            )
        )
    )
    ready_gate, ready_up, scale_gate, scale_up, router = pl.pallas_call(
        write_kernel,
        out_shape=(
            jax.ShapeDtypeStruct((1, X * ROWS, COLS), bf16),
            jax.ShapeDtypeStruct((1, X * ROWS, COLS), bf16),
            jax.ShapeDtypeStruct((1, COLS), f32),
            jax.ShapeDtypeStruct((1, COLS), f32),
            jax.ShapeDtypeStruct((2 * Y * Z, X * ROWS), bf16),
        ),
        in_specs=[vmem] * 3,
        out_specs=(hbm,) * 5,
        scratch_shapes=[dma, dma, dma],
        compiler_params=pltpu.CompilerParams(vmem_limit_bytes=1024 * 1024),
        name="write",
    )(*(pltpu.with_memory_space_constraint(a, pltpu.VMEM) for a in (out, sc, rout)))
    return ready_gate, ready_up, scale_gate, scale_up, router.T


def solution(mesh):
    placed = (
        P("ep", "fsdp", None),
        P("ep", "fsdp", None),
        P("ep", "fsdp", None),
        P("ep", "fsdp", None),
        P("ep"),
        P("fsdp", "ep"),
        P("fsdp"),
    )
    return jax.shard_map(
        per_device,
        mesh=mesh,
        in_specs=placed,
        out_specs=(P("ep", None, None), P("ep", None, None), P("ep", None), P("ep", None), P()),
        check_vma=False,
    )
```
